32 devices in a mesh: lon: 8 (over y, x, core), lat: 4 (over z).
Axes of the slice: x: 2, y: 2, z: 4, core: 2. Of those that a mesh axis runs over, the one named last changes fastest.
Arguments:
- grid_latent: bfloat16 [4, 8, 1024, 512], P('lat', 'lon'), may hold values from -6 to 6
- mesh_latent: bfloat16 [4, 8, 160, 512], P('lat', 'lon'), may hold values from -6 to 6
- edge_geometry: float32 [4, 8, 4, 2048], P('lat', 'lon'), may hold values from -6 to 6
- senders: int32 [4, 8, 2048], P('lat', 'lon'), may hold values from 0 to 1023
- receivers: int32 [4, 8, 2048], P('lat', 'lon'), may hold values from 0 to 1439, as said below
- w_grid: bfloat16 [512, 512], replicated, may hold values from -0.25 to 0.25
- w_mesh: bfloat16 [512, 512], replicated, may hold values from -0.25 to 0.25
- w_edge: float32 [4, 512], replicated, may hold values from -3 to 3
- edge_bias: float32 [512], replicated, may hold values from -3 to 3
- w_message: bfloat16 [512, 512], replicated, may hold values from -0.25 to 0.25
- w_node: bfloat16 [1024, 512], replicated, may hold values from -0.1875 to 0.1875
- w_output: bfloat16 [512, 512], replicated, may hold values from -0.25 to 0.25
- norm_gain: float32 [512], replicated, may hold values from 0.1 to 1.9
- norm_bias: float32 [512], replicated, may hold values from -3 to 3
Outputs:
- mesh_out: bfloat16 [4, 8, 160, 512], P('lat', 'lon')
The draws below stay inside these ranges and needn't reach their ends.
Inputs may be any that keep to these rules, and one draw needn't show every extreme that they name: `receivers`: r // 160 is a neighbour slot s from 0 to 8 (latitude offset s // 3 - 1, longitude offset s % 3 - 1); edges of the first band never name latitude offset -1, those of the last band never +1. For s other than 4, with k = s for s < 4 and k = s - 1 otherwise, the row r % 160 lies in k * 16 to k * 16 + 15 for s = 1, 3, 5, 7 and in k * 16 to k * 16 + 3 for s = 0, 2, 6, 8.
All inputs are finite; a program needn't handle non-finite values.
Results may differ from the reference program's by a relative error of at most 0.0095.
Values may be sent and summed in bfloat16 or wider, within the bound.
A program may use at most 64 MiB of HBM per device.

```python
import jax
import jax.numpy as jnp
from jax import lax

D = 512
M_DEV = 160
B_SIDE = 16
B_CORNER = 4
G_DEV = 1024
E_DEV = 2048
N_LON = 8
N_LAT = 4


def draw_receivers(key, part):
    base = jax.random.fold_in(key, 11)
    key_slot, key_side, key_corner, key_own = jax.random.split(base, 4)
    array_shape = (N_LAT, N_LON, E_DEV)
    raw_slot = jax.random.randint(key_slot, array_shape, 0, 40)
    neighbour = raw_slot - 32
    neighbour = neighbour + (neighbour >= 4).astype(jnp.int32)
    slot_number = jnp.where(raw_slot < 32, 4, neighbour)
    band_index = jnp.arange(N_LAT, dtype=jnp.int32)[:, None, None]
    lat_offset = slot_number // 3
    outside = (band_index == 0) & (lat_offset == 0) | (band_index == N_LAT - 1) & (lat_offset == 2)
    slot_number = jnp.where(outside, 3 + slot_number % 3, slot_number)
    side_row = jax.random.randint(key_side, array_shape, 0, B_SIDE)
    corner_row = jax.random.randint(key_corner, array_shape, 0, B_CORNER)
    own_row = jax.random.randint(key_own, array_shape, 0, M_DEV)
    strip_number = jnp.where(slot_number < 4, slot_number, slot_number - 1)
    is_corner = (slot_number % 2 == 0) & (slot_number != 4)
    border_row = strip_number * B_SIDE + jnp.where(is_corner, corner_row, side_row)
    row_number = jnp.where(slot_number == 4, own_row, border_row)
    return (slot_number * M_DEV + row_number).astype(jnp.int32)


def plant(drawn, own_key, least, high):
    place = [jax.random.randint(jax.random.fold_in(own_key, axis), (), 0, length) for axis, length in enumerate(drawn.shape)]
    main_axis = drawn.shape.index(max(drawn.shape))
    beside = place[:main_axis] + [(place[main_axis] + 1) % drawn.shape[main_axis]] + place[main_axis + 1:]
    return drawn.at[tuple(place)].set(least).at[tuple(beside)].set(high)


def levels(own_key, dims, cuts, least, top_value):
    level = 1.0
    for position, parts in cuts:
        draws = jax.random.uniform(jax.random.fold_in(jax.random.fold_in(own_key, 6), position), (parts,), jnp.float32, least / len(cuts), top_value / len(cuts))
        level = level * jnp.repeat(jnp.exp(draws), dims[position] // parts).reshape((-1,) + (1,) * (len(dims) - 1 - position))
    return level


def scatter_about(rng, extent, spread, bound, cuts=(), kind=jnp.bfloat16):
    level = levels(rng, extent, cuts, -0.22, 0.18) if cuts else 1.0
    result = jax.random.normal(rng, extent, jnp.float32) * spread * level
    return jnp.minimum(jnp.maximum(result, -bound), bound).astype(kind)


def setup_inputs(seed: int = 0) -> dict:
    seeds = jax.random.split(jax.random.key(seed), 15)
    return {
        "grid_latent": scatter_about(seeds[0], (N_LAT, N_LON, G_DEV, D), 1.0, 6.0, ((0, 4), (1, 8))),
        "mesh_latent": scatter_about(seeds[1], (N_LAT, N_LON, M_DEV, D), 1.0, 6.0, ((0, 4), (1, 8))),
        "edge_geometry": scatter_about(seeds[2], (N_LAT, N_LON, 4, E_DEV), 1.0, 6.0, ((0, 4), (1, 8)), jnp.float32),
        "senders": plant(jax.random.randint(seeds[3], (N_LAT, N_LON, E_DEV), 0, G_DEV), jax.random.fold_in(seeds[3], 1), 0, G_DEV - 1).astype(jnp.int32),
        "receivers": draw_receivers(jax.random.fold_in(seeds[14], 71), 0),
        "w_grid": scatter_about(seeds[5], (D, D), D ** -0.5, 0.25),
        "w_mesh": scatter_about(seeds[6], (D, D), D ** -0.5, 0.25),
        "w_edge": scatter_about(seeds[7], (4, D), 4 ** -0.5, 3.0, (), jnp.float32),
        "edge_bias": scatter_about(seeds[8], (D,), 0.5, 3.0, (), jnp.float32),
        "w_message": scatter_about(seeds[9], (D, D), D ** -0.5, 0.25),
        "w_node": scatter_about(seeds[10], (2 * D, D), (2 * D) ** -0.5, 0.1875),
        "w_output": scatter_about(seeds[11], (D, D), D ** -0.5, 0.25),
        "norm_gain": jnp.clip(1.0 + 0.18 * jax.random.normal(seeds[12], (D,), jnp.float32), 0.1, 1.9),
        "norm_bias": scatter_about(seeds[13], (D,), 0.5, 3.0, (), jnp.float32),
    }


def reference(grid_latent, mesh_latent, edge_geometry, senders, receivers, w_grid, w_mesh, w_edge, edge_bias, w_message, w_node, w_output, norm_gain, norm_bias):
    features = mesh_latent.shape[-1]
    mesh_flat = mesh_latent.reshape(-1, features)
    mesh_proj = jnp.dot(mesh_flat, w_mesh, preferred_element_type=jnp.float32)
    lon_index = jnp.arange(N_LON, dtype=jnp.int32)[:, None]

    def one_band(summed, items):
        band_grid, band_senders, band_receivers, band_geometry, band_index = items
        grid_proj = jnp.dot(band_grid.reshape(-1, features), w_grid, preferred_element_type=jnp.float32)
        grid_proj = grid_proj.reshape(N_LON, G_DEV, features)
        gathered = jax.vmap(lambda table, picks: jnp.take(table, picks, axis=0))(grid_proj, band_senders)
        slot_number = band_receivers // M_DEV
        row_number = band_receivers % M_DEV
        target_lat = band_index + slot_number // 3 - 1
        target_lon = (lon_index + slot_number % 3 - 1) % N_LON
        node_ids = ((target_lat * N_LON + target_lon) * M_DEV + row_number).astype(jnp.int32)
        geometry = jnp.einsum('lce,cd->led', band_geometry, w_edge, precision=lax.Precision.HIGHEST)
        preact = gathered + jnp.take(mesh_proj, node_ids, axis=0) + geometry + edge_bias
        hidden = jax.nn.silu(preact).astype(jnp.bfloat16)
        message = jnp.dot(hidden.reshape(-1, features), w_message, preferred_element_type=jnp.float32).astype(jnp.bfloat16)
        summed = summed + jax.ops.segment_sum(message.astype(jnp.float32), node_ids.reshape(-1), num_segments=mesh_flat.shape[0])
        return (summed, None)
    bands = jnp.arange(N_LAT, dtype=jnp.int32)
    start = jnp.zeros(mesh_flat.shape, jnp.float32)
    aggregated, _ = lax.scan(one_band, start, (grid_latent, senders, receivers, edge_geometry, bands))
    node_in = jnp.concatenate([mesh_flat, aggregated.astype(jnp.bfloat16)], axis=1)
    node_hidden = jax.nn.silu(jnp.dot(node_in, w_node, preferred_element_type=jnp.float32)).astype(jnp.bfloat16)
    update = jnp.dot(node_hidden, w_output, preferred_element_type=jnp.float32)
    row_mean = lax.optimization_barrier(jnp.mean(update, axis=-1, keepdims=True))
    centered = update - row_mean
    row_var = lax.optimization_barrier(jnp.mean(centered * centered, axis=-1, keepdims=True))
    normed = centered * lax.rsqrt(row_var + 1e-05) * norm_gain + norm_bias
    mesh_out = (mesh_flat.astype(jnp.float32) + normed).astype(jnp.bfloat16)
    return mesh_out.reshape(mesh_latent.shape)
```

```python
import functools

import jax
import jax.numpy as jnp
from jax import lax
from jax.experimental import pallas as pl
from jax.experimental.pallas import tpu as pltpu
from jax.sharding import PartitionSpec as P

B_SIDE = 16
B_CORNER = 4
BLOCK = 8
LANES = 128
DIGIT = 256
CHUNK = 512
SIDES_AT = 0
CORNERS_AT = 1
MESH = pl.DeviceIdType.MESH

BF16 = jnp.bfloat16
F32 = jnp.float32

SIDES = (1, 3, 5, 7)
CORNERS = (0, 2, 6, 8)


def strip(slot):
    return slot if slot < 4 else slot - 1


def nn(a, b):
    return jnp.dot(a, b, preferred_element_type=F32)


def halves(x):
    high = x.astype(BF16)
    return high, (x - high.astype(F32)).astype(BF16)


def down(row, count):
    return jnp.transpose(jnp.broadcast_to(row, (count, row.shape[1])))


def equal(a, b):
    one = jnp.ones(a.shape, BF16)
    return jnp.where(a == b, one, jnp.zeros_like(one))


def kernel(
    n_lon,
    n_lat,
    grid_h,
    mesh_h,
    geo_h,
    snd_h,
    rcv_h,
    w_grid_h,
    w_mesh_h,
    w_edge_h,
    bias_h,
    w_message_h,
    w_node_h,
    w_output_h,
    gain_h,
    nbias_h,
    out_ref,
    grid_v,
    mesh_v,
    geo_v,
    snd_v,
    rcv_v,
    w_grid_v,
    w_mesh_v,
    w_edge_v,
    bias_v,
    w_message_v,
    w_node_v,
    w_output_v,
    gain_v,
    nbias_v,
    table,
    edge_table,
    picks_e,
    picks_n,
    before,
    put_sum,
    got_sum,
    load_sem,
    send_sem,
    recv_sem,
    ready_sem,
):
    lon = lax.axis_index("lon")
    lat = lax.axis_index("lat")
    rows, features = mesh_v.shape
    grid_rows = grid_v.shape[0]
    edges = snd_v.shape[1]
    corner_base = rows + 4 * B_SIDE
    slots = corner_base + 4 * BLOCK
    cut = rows // LANES * LANES
    border = 8 * B_SIDE

    def there(dlat, dlon):
        return {
            "lat": lat + dlat,
            "lon": lax.rem(lon + dlon + n_lon, n_lon),
        }

    def guarded(dlat, body):
        if dlat == 0:
            body()
        else:
            pl.when(lat > 0 if dlat < 0 else lat < n_lat - 1)(body)

    groups = [
        [(snd_h.at[0], snd_v)],
        [(w_grid_h, w_grid_v), (grid_h.at[0, 0], grid_v)],
        [
            (mesh_h.at[0, 0], mesh_v),
            (w_mesh_h, w_mesh_v),
            (rcv_h.at[0], rcv_v),
            (geo_h.at[0, 0], geo_v),
            (w_edge_h, w_edge_v),
        ],
        [(bias_h, bias_v), (gain_h, gain_v), (nbias_h, nbias_v)],
        [(w_message_h, w_message_v), (w_node_h, w_node_v), (w_output_h, w_output_v)],
    ]
    for number, group in enumerate(groups):
        for source, target in group:
            pltpu.make_async_copy(source, target, load_sem.at[number]).start()

    def bytes_of(ref):
        return ref.dtype.itemsize * functools.reduce(lambda a, b: a * b, ref.shape)

    def span_of(total):
        if total < bytes_of(snd_v):
            return snd_v.at[:, pl.ds(0, total // snd_v.dtype.itemsize)]
        if total < bytes_of(table):
            return table.at[pl.ds(0, total // (2 * features))]
        return before.at[pl.ds(0, total // (4 * features))]

    def loaded(number):
        view = span_of(sum(bytes_of(target) for _, target in groups[number]))
        pltpu.make_async_copy(view, view, load_sem.at[number]).wait()

    edge_table[...] = jnp.zeros(edge_table.shape, BF16)
    got_sum[...] = jnp.zeros(got_sum.shape, BF16)

    barrier = pltpu.get_barrier_semaphore()

    def greet(dlat, dlon):
        pl.semaphore_signal(barrier, inc=1, device_id=there(dlat, dlon), device_id_type=MESH)

    greet(0, -1)
    greet(0, 1)
    guarded(-1, lambda: greet(-1, 0))
    guarded(1, lambda: greet(1, 0))

    def offset(slot):
        return slot // 3 - 1, slot % 3 - 1

    def place(slot):
        if slot in SIDES:
            return rows + B_SIDE * SIDES.index(slot)
        return corner_base + BLOCK * CORNERS.index(slot)

    def size_of(slot):
        return B_SIDE if slot in SIDES else B_CORNER

    def mesh_copy(slot):
        dlat, dlon = offset(slot)
        size = size_of(slot)
        return pltpu.make_async_remote_copy(
            src_ref=table.at[pl.ds(grid_rows + strip(slot) * B_SIDE, size)],
            dst_ref=edge_table.at[pl.ds(place(slot) - cut, size)],
            send_sem=send_sem.at[1 - dlat],
            recv_sem=recv_sem.at[1 + dlat],
            device_id=there(-dlat, -dlon),
            device_id_type=MESH,
        )

    def sum_copy(slot):
        dlat, dlon = offset(slot)
        size = size_of(slot)
        return pltpu.make_async_remote_copy(
            src_ref=put_sum.at[pl.ds(place(slot) - rows, size)],
            dst_ref=got_sum.at[pl.ds(strip(slot) * B_SIDE, size)],
            send_sem=send_sem.at[4 + dlat],
            recv_sem=recv_sem.at[4 - dlat],
            device_id=there(dlat, dlon),
            device_id_type=MESH,
        )

    def settle(sems, first):
        for dlat in (-1, 1, 0):

            def body(dlat=dlat):
                count = sum(size_of(s) for s in SIDES + CORNERS if offset(s)[0] == dlat)
                view = table.at[pl.ds(0, count)]
                pltpu.make_async_copy(view, view, sems.at[first + 1 + dlat]).wait()

            guarded(dlat, body)

    def each(chosen, sign, action):
        for dlat in (-1, 1, 0):
            members = [s for s in chosen if offset(s)[0] == sign * dlat]
            if members:

                def body(members=members):
                    for s in members:
                        action(s)

                guarded(dlat, body)

    def send_sides():
        arrivals = 2 + (lat > 0).astype(jnp.int32) + (lat < n_lat - 1).astype(jnp.int32)
        pl.semaphore_wait(barrier, arrivals)
        each(SIDES, -1, lambda s: mesh_copy(s).start())
        for dlat in (-1, 1):

            def tell(dlat=dlat):
                pl.semaphore_signal(
                    ready_sem.at[0 if dlat > 0 else 1],
                    inc=1,
                    device_id=there(dlat, 0),
                    device_id_type=MESH,
                )

            guarded(dlat, tell)

    def send_corners():
        for dlat in (-1, 1):

            def go(dlat=dlat):
                pl.semaphore_wait(ready_sem.at[0 if dlat < 0 else 1], 1)
                for s in CORNERS:
                    if offset(s)[0] == -dlat:
                        mesh_copy(s).start()

            guarded(dlat, go)

    step = min(CHUNK, edges)
    starts = list(range(0, edges, step))
    digits = grid_rows // DIGIT
    lane = lax.broadcasted_iota(jnp.int32, (step, LANES), 1).astype(F32)
    lanes = [(lane + float(LANES * h)).astype(BF16) for h in range(DIGIT // LANES)]

    loaded(0)
    senders = snd_v[...]
    upper = lax.shift_left(lax.shift_right_logical(senders, 8), 8)
    lower = (senders - upper).astype(F32).astype(BF16)
    upper = upper.astype(F32).astype(BF16)
    loaded(1)
    table[:grid_rows, :] = (0.5 * nn(grid_v[...], w_grid_v[...])).astype(BF16)
    for start in starts:
        span = pl.ds(start, step)
        low = down(lower[:, start : start + step], LANES)
        high = down(upper[:, start : start + step], LANES)
        for q in range(digits):
            digit = (high - float(DIGIT * q)) + low
            for h in range(DIGIT // LANES):
                picks_e[span, pl.ds(q * DIGIT + h * LANES, LANES)] = equal(digit, lanes[h])

    loaded(2)
    loaded(3)
    high, low = [part.astype(F32) for part in halves(w_edge_v[...])]
    bias_high, bias_low = [part.astype(F32) for part in halves(bias_v[...])]
    blank = jnp.zeros((BLOCK - B_CORNER, features), F32)
    last = jnp.concatenate(
        [bias_high, bias_low, jnp.zeros((B_CORNER - 2, features), F32)], 0
    )
    own = nn(mesh_v[...], w_mesh_v[...])
    table[grid_rows:, :] = (
        0.5
        * jnp.concatenate(
            [own, jnp.zeros((corner_base - rows, features), F32)]
            + [blank, high, blank, low, blank, high, blank, last],
            0,
        )
    ).astype(BF16)

    picks = rcv_v[...]
    shift, spot = 0, picks
    for s in range(9):
        base = (0 if s == 4 else place(s) - strip(s) * B_SIDE) - s * rows
        if s == 0:
            spot = spot + base
        else:
            spot = spot + jnp.where(picks >= s * rows, base - shift, 0)
        shift = base
    spot = spot.astype(F32).astype(BF16)
    high, low = [part.astype(F32) for part in halves(geo_v[...])]
    empty = jnp.zeros((BLOCK - B_CORNER, edges), F32)
    ones = jnp.concatenate([jnp.ones((2, edges), F32), jnp.zeros((2, edges), F32)], 0)
    tail = jnp.concatenate(
        [jnp.zeros((corner_base - cut, edges), F32)]
        + [empty, high, empty, high, empty, low, empty, ones],
        0,
    ).astype(BF16)
    for start in starts:
        span = pl.ds(start, step)
        at = down(spot[:, start : start + step], LANES)
        for h in range(slots // LANES):
            found = equal(at, lanes[h])
            if h * LANES == cut:
                found = found + jnp.transpose(tail[:, start : start + step])
            picks_e[span, pl.ds(grid_rows + h * LANES, LANES)] = found
    row = lax.broadcasted_iota(jnp.int32, (slots, step), 0).astype(F32).astype(BF16)
    for start in starts:
        at = jnp.broadcast_to(spot[:, start : start + step], (slots, step))
        picks_n[:, pl.ds(start, step)] = equal(row, at)

    for number, start in enumerate(starts):
        if number == SIDES_AT:
            send_sides()
        if number == CORNERS_AT:
            send_corners()
        span = pl.ds(start, step)
        before[span, :] = nn(picks_e[span, :], table[...])

    settle(recv_sem, 0)

    summed = None
    for start in starts:
        span = pl.ds(start, step)
        half = before[span, :] + nn(picks_e[span, grid_rows + cut :], edge_table[...])
        hidden = (half + half * jnp.tanh(half)).astype(BF16)
        added = nn(picks_n[:, span], hidden)
        summed = added if summed is None else summed + added

    put_sum[...] = summed[rows:, :].astype(BF16)
    each(SIDES + CORNERS, 1, lambda s: sum_copy(s).start())

    loaded(4)
    fold = nn(w_message_v[...], w_node_v[features:, :]).astype(BF16)
    high, low = halves(summed[:rows, :])
    node = nn(mesh_v[...], w_node_v[:features, :]) + nn(high, fold) + nn(low, fold)

    def finish(node, span):
        node_hidden = (node * jax.nn.sigmoid(node)).astype(BF16)
        update = nn(node_hidden, w_output_v[...])
        row_mean = jnp.mean(update, axis=-1, keepdims=True)
        centered = update - row_mean
        row_var = jnp.mean(centered * centered, axis=-1, keepdims=True)
        normed = centered * lax.rsqrt(row_var + 1e-05) * gain_v[...] + nbias_v[...]
        out_ref[0, 0, span, :] = (mesh_v[span, :].astype(F32) + normed).astype(BF16)

    finish(node[border:], pl.ds(border, rows - border))
    settle(recv_sem, 3)
    finish(node[:border] + nn(got_sum[...], fold), pl.ds(0, border))

    settle(send_sem, 0)
    settle(send_sem, 3)


def local(n_lon, n_lat, *args):
    args = [a.reshape(1, -1) if a.ndim == 1 else a for a in args]
    grid_latent, mesh_latent, geometry, senders = args[:4]
    rows, features = mesh_latent.shape[2:]
    grid_rows = grid_latent.shape[2]
    edges = senders.shape[2]
    slots = rows + 4 * B_SIDE + 4 * BLOCK
    cut = rows // LANES * LANES
    loads = []
    for number, a in enumerate(args):
        shape = a.shape[2:] if number < 3 else a.shape[1:] if number < 5 else a.shape
        loads.append(pltpu.VMEM(shape, a.dtype))
    return pl.pallas_call(
        functools.partial(kernel, n_lon, n_lat),
        out_shape=pltpu.VMEM(mesh_latent.shape, BF16),
        in_specs=[pl.BlockSpec(memory_space=pl.ANY)] * len(args),
        out_specs=pl.BlockSpec(memory_space=pltpu.VMEM),
        scratch_shapes=loads
        + [
            pltpu.VMEM((grid_rows + slots, features), BF16),
            pltpu.VMEM((slots - cut, features), BF16),
            pltpu.VMEM((edges, grid_rows + slots), BF16),
            pltpu.VMEM((slots, edges), BF16),
            pltpu.VMEM((edges, features), F32),
            pltpu.VMEM((slots - rows, features), BF16),
            pltpu.VMEM((8 * B_SIDE, features), BF16),
            pltpu.SemaphoreType.DMA((5,)),
            pltpu.SemaphoreType.DMA((6,)),
            pltpu.SemaphoreType.DMA((6,)),
            pltpu.SemaphoreType.REGULAR((2,)),
        ],
        compiler_params=pltpu.CompilerParams(
            collective_id=0, has_side_effects=True, vmem_limit_bytes=56 * 1024 * 1024
        ),
    )(*args)


def solution(mesh):
    return jax.shard_map(
        functools.partial(local, mesh.shape["lon"], mesh.shape["lat"]),
        mesh=mesh,
        in_specs=(
            P("lat", "lon", None, None),
            P("lat", "lon", None, None),
            P("lat", "lon", None, None),
            P("lat", "lon", None),
            P("lat", "lon", None),
            P(),
            P(),
            P(),
            P(),
            P(),
            P(),
            P(),
            P(),
            P(),
        ),
        out_specs=P("lat", "lon", None, None),
        check_vma=False,
    )
```

```python
import functools

import jax
import jax.numpy as jnp
from jax import lax
from jax.experimental import pallas as pl
from jax.experimental.pallas import tpu as pltpu
from jax.sharding import PartitionSpec as P

B_SIDE = 16
B_CORNER = 4
BLOCK = 8
LANES = 128
DIGIT = 256
CHUNK = 256
UP_AT = 1
MESH = pl.DeviceIdType.MESH

BF16 = jnp.bfloat16
F32 = jnp.float32

SIDES = (1, 3, 5, 7)
CORNERS = (0, 2, 6, 8)


def strip(slot):
    return slot if slot < 4 else slot - 1


def nn(a, b):
    return jnp.dot(a, b, preferred_element_type=F32)


def halves(x):
    high = x.astype(BF16)
    return high, (x - high.astype(F32)).astype(BF16)


def down(row, count):
    return jnp.transpose(jnp.broadcast_to(row, (count, row.shape[1])))


def equal(a, b):
    one = jnp.ones(a.shape, BF16)
    return jnp.where(a == b, one, jnp.zeros_like(one))


def kernel(
    n_lon,
    n_lat,
    grid_h,
    mesh_h,
    geo_h,
    snd_h,
    rcv_h,
    w_grid_h,
    w_mesh_h,
    w_edge_h,
    bias_h,
    w_message_h,
    w_node_h,
    w_output_h,
    gain_h,
    nbias_h,
    out_ref,
    grid_v,
    mesh_v,
    geo_v,
    snd_v,
    rcv_v,
    w_grid_v,
    w_mesh_v,
    w_edge_v,
    bias_v,
    w_message_v,
    w_node_v,
    w_output_v,
    gain_v,
    nbias_v,
    table,
    edge_table,
    low_v,
    high_v,
    spot_v,
    tail_v,
    before,
    put_sum,
    got_sum,
    w_center,
    node_v,
    load_sem,
    send_sem,
    recv_sem,
    ready_sem,
):
    lon = lax.axis_index("lon")
    lat = lax.axis_index("lat")
    rows, features = mesh_v.shape
    grid_rows = grid_v.shape[0]
    edges = snd_v.shape[1]
    corner_base = rows + 4 * B_SIDE
    slots = corner_base + 4 * BLOCK
    cut = rows // LANES * LANES
    border = 8 * B_SIDE

    def there(dlat, dlon):
        return {
            "lat": lat + dlat,
            "lon": lax.rem(lon + dlon + n_lon, n_lon),
        }

    def guarded(dlat, body):
        if dlat == 0:
            body()
        else:
            pl.when(lat > 0 if dlat < 0 else lat < n_lat - 1)(body)

    edge_table[...] = jnp.zeros(edge_table.shape, BF16)
    got_sum[...] = jnp.zeros(got_sum.shape, BF16)

    barrier = pltpu.get_barrier_semaphore()

    def greet(dlat, dlon):
        pl.semaphore_signal(barrier, inc=1, device_id=there(dlat, dlon), device_id_type=MESH)

    greet(0, -1)
    greet(0, 1)
    guarded(-1, lambda: greet(-1, 0))
    guarded(1, lambda: greet(1, 0))

    groups = [
        [(snd_h.at[0], snd_v)],
        [
            (mesh_h.at[0, 0], mesh_v),
            (w_mesh_h, w_mesh_v),
            (w_edge_h, w_edge_v),
            (rcv_h.at[0], rcv_v),
            (geo_h.at[0, 0], geo_v),
        ],
        [(bias_h, bias_v), (gain_h, gain_v), (nbias_h, nbias_v)],
        [(w_grid_h, w_grid_v), (grid_h.at[0, 0], grid_v)],
        [(w_message_h, w_message_v), (w_node_h, w_node_v), (w_output_h, w_output_v)],
    ]

    def load(number):
        for source, target in groups[number]:
            pltpu.make_async_copy(source, target, load_sem.at[number]).start()

    for number in range(4):
        load(number)

    def bytes_of(ref):
        return ref.dtype.itemsize * functools.reduce(lambda a, b: a * b, ref.shape)

    def span_of(total):
        if total < bytes_of(snd_v):
            return snd_v.at[:, pl.ds(0, total // snd_v.dtype.itemsize)]
        if total < bytes_of(table):
            return table.at[pl.ds(0, total // (2 * features))]
        return before.at[pl.ds(0, total // (4 * features))]

    def loaded(number):
        view = span_of(sum(bytes_of(target) for _, target in groups[number]))
        pltpu.make_async_copy(view, view, load_sem.at[number]).wait()

    def offset(slot):
        return slot // 3 - 1, slot % 3 - 1

    def place(slot):
        if slot in SIDES:
            return rows + B_SIDE * SIDES.index(slot)
        return corner_base + BLOCK * CORNERS.index(slot)

    def size_of(slot):
        return B_SIDE if slot in SIDES else B_CORNER

    def mesh_copy(slot):
        dlat, dlon = offset(slot)
        size = size_of(slot)
        return pltpu.make_async_remote_copy(
            src_ref=table.at[pl.ds(grid_rows + strip(slot) * B_SIDE, size)],
            dst_ref=edge_table.at[pl.ds(place(slot) - cut, size)],
            send_sem=send_sem.at[1 - dlat],
            recv_sem=recv_sem.at[1 + dlat],
            device_id=there(-dlat, -dlon),
            device_id_type=MESH,
        )

    def sum_copy(slot):
        dlat, dlon = offset(slot)
        size = size_of(slot)
        return pltpu.make_async_remote_copy(
            src_ref=put_sum.at[pl.ds(place(slot) - rows, size)],
            dst_ref=got_sum.at[pl.ds(place(slot) - rows, size)],
            send_sem=send_sem.at[1 + dlat],
            recv_sem=recv_sem.at[4 - dlat],
            device_id=there(dlat, dlon),
            device_id_type=MESH,
        )

    def settle(sems, first, chosen, times=1):
        for dlat in (-1, 1, 0):
            count = times * sum(size_of(s) for s in chosen if offset(s)[0] == dlat)
            if count:

                def body(dlat=dlat, count=count):
                    view = table.at[pl.ds(0, count)]
                    pltpu.make_async_copy(view, view, sems.at[first + 1 + dlat]).wait()

                guarded(dlat, body)

    def each(chosen, sign, action):
        for dlat in (-1, 1, 0):
            members = [s for s in chosen if offset(s)[0] == sign * dlat]
            if members:

                def body(members=members):
                    for s in members:
                        action(s)

                guarded(dlat, body)

    def send_sides():
        arrivals = 2 + (lat > 0).astype(jnp.int32) + (lat < n_lat - 1).astype(jnp.int32)
        pl.semaphore_wait(barrier, arrivals)
        for dlat in (-1, 1):

            def tell(dlat=dlat):
                pl.semaphore_signal(
                    ready_sem.at[0 if dlat > 0 else 1],
                    inc=1,
                    device_id=there(dlat, 0),
                    device_id_type=MESH,
                )

            guarded(dlat, tell)
        each(SIDES, -1, lambda s: mesh_copy(s).start())

    def send_corners(dlat):
        def go():
            pl.semaphore_wait(ready_sem.at[0 if dlat < 0 else 1], 1)
            for s in CORNERS:
                if offset(s)[0] == -dlat:
                    mesh_copy(s).start()

        guarded(dlat, go)

    step = min(CHUNK, edges)
    starts = list(range(0, edges, step))
    digits = grid_rows // DIGIT
    lane = lax.broadcasted_iota(jnp.int32, (step, LANES), 1).astype(F32)
    lanes = [(lane + float(LANES * h)).astype(BF16) for h in range(DIGIT // LANES)]

    loaded(0)
    senders = snd_v[...]
    upper = lax.shift_left(lax.shift_right_logical(senders, 8), 8)
    lower = (senders - upper).astype(F32).astype(BF16)
    upper = upper.astype(F32).astype(BF16)

    for start in starts:
        span = pl.ds(start, step)
        low_v[span, :] = down(lower[:, start : start + step], LANES)
        high_v[span, :] = down(upper[:, start : start + step], LANES)

    loaded(1)
    loaded(2)
    high, low = [part.astype(F32) for part in halves(w_edge_v[...])]
    bias_high, bias_low = [part.astype(F32) for part in halves(bias_v[...])]
    blank = jnp.zeros((BLOCK - B_CORNER, features), F32)
    last = jnp.concatenate(
        [bias_high, bias_low, jnp.zeros((B_CORNER - 2, features), F32)], 0
    )
    own = nn(mesh_v[...], w_mesh_v[...])
    table[grid_rows:, :] = (
        0.5
        * jnp.concatenate(
            [own, jnp.zeros((corner_base - rows, features), F32)]
            + [blank, high, blank, low, blank, high, blank, last],
            0,
        )
    ).astype(BF16)
    send_sides()
    picks = rcv_v[...]
    shift, spot = 0, picks
    for s in range(9):
        base = (0 if s == 4 else place(s) - strip(s) * B_SIDE) - s * rows
        if s == 0:
            spot = spot + base
        else:
            spot = spot + jnp.where(picks >= s * rows, base - shift, 0)
        shift = base
    spot = spot.astype(F32).astype(BF16)
    high, low = [part.astype(F32) for part in halves(geo_v[...])]
    empty = jnp.zeros((BLOCK - B_CORNER, edges), F32)
    ones = jnp.concatenate([jnp.ones((2, edges), F32), jnp.zeros((2, edges), F32)], 0)
    tail = jnp.concatenate(
        [jnp.zeros((corner_base - cut, edges), F32)]
        + [empty, high, empty, high, empty, low, empty, ones],
        0,
    ).astype(BF16)
    for start in starts:
        span = pl.ds(start, step)
        spot_v[span, :] = down(spot[:, start : start + step], LANES)
        tail_v[span, :] = jnp.transpose(tail[:, start : start + step])

    send_corners(-1)
    loaded(3)
    load(4)
    table[:grid_rows, :] = (0.5 * nn(grid_v[...], w_grid_v[...])).astype(BF16)

    def picked(span, first):
        tiles = []
        for h in range(first, slots // LANES):
            found = equal(spot_v[span, :], lanes[h])
            tiles.append(found + tail_v[span, :] if h * LANES == cut else found)
        return tiles

    for number, start in enumerate(starts):
        if number == UP_AT:
            send_corners(1)
        span = pl.ds(start, step)
        tiles = []
        for q in range(digits):
            digit = (high_v[span, :] - float(DIGIT * q)) + low_v[span, :]
            tiles += [equal(digit, lanes[h]) for h in range(DIGIT // LANES)]
        before[span, :] = nn(jnp.concatenate(tiles + picked(span, 0), 1), table[...])

    settle(recv_sem, 0, SIDES + CORNERS)

    parts = []
    for start in starts:
        span = pl.ds(start, step)
        tiles = picked(span, cut // LANES)
        half = before[span, :] + nn(jnp.concatenate(tiles, 1), edge_table[...])
        parts.append((half + half * jnp.tanh(half)).astype(BF16))
    row = lax.broadcasted_iota(jnp.int32, (slots, edges), 0).astype(F32).astype(BF16)
    at = jnp.broadcast_to(spot, (slots, edges))
    summed = nn(equal(row, at), jnp.concatenate(parts, 0))

    put_sum[...] = summed[rows:, :].astype(BF16)
    each(CORNERS, 1, lambda s: sum_copy(s).start())
    each(SIDES, 1, lambda s: sum_copy(s).start())

    loaded(4)
    fold = nn(w_message_v[...], w_node_v[features:, :]).astype(BF16)
    high, low = halves(summed[:rows, :])
    node_v[...] = (
        nn(mesh_v[...], w_node_v[:features, :]) + nn(high, fold) + nn(low, fold)
    )
    weights = w_output_v[...].astype(F32)
    center = jnp.mean(weights, axis=-1, keepdims=True)
    w_center[...] = (weights - center).astype(BF16)

    def rows_of(ref, spans):
        return jnp.concatenate([ref[pl.ds(*span), :].astype(F32) for span in spans], 0)

    def finish(spans, extra=None):
        node = rows_of(node_v, spans)
        if extra is not None:
            node = node + nn(extra[...], fold)
        node_hidden = (node * jax.nn.sigmoid(node)).astype(BF16)
        centered = nn(node_hidden, w_center[...])
        row_var = jnp.mean(centered * centered, axis=-1, keepdims=True)
        normed = centered * lax.rsqrt(row_var + 1e-05) * gain_v[...] + nbias_v[...]
        result = rows_of(mesh_v, spans) + normed
        first = 0
        for start, count in spans:
            out_ref[0, 0, pl.ds(start, count), :] = result[first : first + count].astype(BF16)
            first += count

    at_sides = [(strip(s) * B_SIDE, B_SIDE) for s in SIDES]
    at_corners = [(strip(s) * B_SIDE, BLOCK) for s in CORNERS]
    between = [(strip(s) * B_SIDE + BLOCK, B_SIDE - BLOCK) for s in CORNERS]
    finish([(border, rows - border)] + between)
    settle(recv_sem, 3, SIDES + CORNERS)
    finish(at_sides + at_corners, got_sum)

    settle(send_sem, 0, SIDES + CORNERS, 2)


def local(n_lon, n_lat, *args):
    args = [a.reshape(1, -1) if a.ndim == 1 else a for a in args]
    grid_latent, mesh_latent, geometry, senders = args[:4]
    rows, features = mesh_latent.shape[2:]
    grid_rows = grid_latent.shape[2]
    edges = senders.shape[2]
    slots = rows + 4 * B_SIDE + 4 * BLOCK
    cut = rows // LANES * LANES
    loads = []
    for number, a in enumerate(args):
        shape = a.shape[2:] if number < 3 else a.shape[1:] if number < 5 else a.shape
        loads.append(pltpu.VMEM(shape, a.dtype))
    return pl.pallas_call(
        functools.partial(kernel, n_lon, n_lat),
        out_shape=pltpu.VMEM(mesh_latent.shape, BF16),
        in_specs=[pl.BlockSpec(memory_space=pl.ANY)] * len(args),
        out_specs=pl.BlockSpec(memory_space=pltpu.VMEM),
        scratch_shapes=loads
        + [
            pltpu.VMEM((grid_rows + slots, features), BF16),
            pltpu.VMEM((slots - cut, features), BF16),
            pltpu.VMEM((edges, LANES), BF16),
            pltpu.VMEM((edges, LANES), BF16),
            pltpu.VMEM((edges, LANES), BF16),
            pltpu.VMEM((edges, LANES), BF16),
            pltpu.VMEM((edges, features), F32),
            pltpu.VMEM((slots - rows, features), BF16),
            pltpu.VMEM((slots - rows, features), BF16),
            pltpu.VMEM((features, features), BF16),
            pltpu.VMEM((rows, features), F32),
            pltpu.SemaphoreType.DMA((5,)),
            pltpu.SemaphoreType.DMA((3,)),
            pltpu.SemaphoreType.DMA((6,)),
            pltpu.SemaphoreType.REGULAR((2,)),
        ],
        compiler_params=pltpu.CompilerParams(
            collective_id=0, has_side_effects=True, vmem_limit_bytes=56 * 1024 * 1024
        ),
    )(*args)


def solution(mesh):
    return jax.shard_map(
        functools.partial(local, mesh.shape["lon"], mesh.shape["lat"]),
        mesh=mesh,
        in_specs=(
            P("lat", "lon", None, None),
            P("lat", "lon", None, None),
            P("lat", "lon", None, None),
            P("lat", "lon", None),
            P("lat", "lon", None),
            P(),
            P(),
            P(),
            P(),
            P(),
            P(),
            P(),
            P(),
            P(),
        ),
        out_specs=P("lat", "lon", None, None),
        check_vma=False,
    )
```

```python
import functools

import jax
import jax.numpy as jnp
from jax import lax
from jax.experimental import pallas as pl
from jax.experimental.pallas import tpu as pltpu
from jax.sharding import PartitionSpec as P

B_SIDE = 16
B_CORNER = 4
BLOCK = 8
LANES = 128
DIGIT = 256
CHUNK = 256
UP_AT = 1
MESH = pl.DeviceIdType.MESH

BF16 = jnp.bfloat16
F32 = jnp.float32
F8 = jnp.float8_e4m3fn

SIDES = (1, 3, 5, 7)
CORNERS = (0, 2, 6, 8)
SENT = (2, 1, 0, 3, 5, 7, 8, 6)


def strip(slot):
    return slot if slot < 4 else slot - 1


def nn(a, b):
    return jnp.dot(a, b, preferred_element_type=F32)


def halves(x):
    high = x.astype(BF16)
    return high, (x - high.astype(F32)).astype(BF16)


def down(row, count):
    return jnp.transpose(jnp.broadcast_to(row, (count, row.shape[1])))


def equal(a, b):
    one = jnp.ones(a.shape, BF16)
    return jnp.where(a == b, one, jnp.zeros_like(one))


def kernel(
    n_lon,
    n_lat,
    grid_h,
    mesh_h,
    geo_h,
    snd_h,
    rcv_h,
    w_grid_h,
    w_mesh_h,
    w_edge_h,
    bias_h,
    w_message_h,
    w_node_h,
    w_output_h,
    gain_h,
    nbias_h,
    out_ref,
    grid_v,
    mesh_v,
    geo_v,
    snd_v,
    rcv_v,
    w_grid_v,
    w_mesh_v,
    w_edge_v,
    bias_v,
    w_message_v,
    w_node_v,
    w_output_v,
    gain_v,
    nbias_v,
    table,
    edge_table,
    low_v,
    high_v,
    picks_8,
    before,
    put_sum,
    got_sum,
    w_center,
    node_v,
    load_sem,
    send_sem,
    recv_sem,
    ready_sem,
):
    lon = lax.axis_index("lon")
    lat = lax.axis_index("lat")
    rows, features = mesh_v.shape
    grid_rows = grid_v.shape[0]
    edges = snd_v.shape[1]
    corner_base = rows + 4 * B_SIDE
    slots = corner_base + 4 * BLOCK
    cut = rows // LANES * LANES
    border = 8 * B_SIDE

    def there(dlat, dlon):
        return {
            "lat": lat + dlat,
            "lon": lax.rem(lon + dlon + n_lon, n_lon),
        }

    def guarded(dlat, body):
        if dlat == 0:
            body()
        else:
            pl.when(lat > 0 if dlat < 0 else lat < n_lat - 1)(body)

    edge_table[...] = jnp.zeros(edge_table.shape, BF16)
    got_sum[...] = jnp.zeros(got_sum.shape, BF16)

    barrier = pltpu.get_barrier_semaphore()

    def greet(dlat, dlon):
        pl.semaphore_signal(barrier, inc=1, device_id=there(dlat, dlon), device_id_type=MESH)

    greet(0, -1)
    greet(0, 1)
    guarded(-1, lambda: greet(-1, 0))
    guarded(1, lambda: greet(1, 0))

    groups = [
        [(snd_h.at[0], snd_v)],
        [
            (mesh_h.at[0, 0], mesh_v),
            (w_mesh_h, w_mesh_v),
            (w_edge_h, w_edge_v),
            (rcv_h.at[0], rcv_v),
            (geo_h.at[0, 0], geo_v),
        ],
        [(bias_h, bias_v), (gain_h, gain_v), (nbias_h, nbias_v)],
        [(w_grid_h, w_grid_v), (grid_h.at[0, 0], grid_v)],
        [(w_message_h, w_message_v), (w_node_h, w_node_v), (w_output_h, w_output_v)],
    ]

    def load(number):
        for source, target in groups[number]:
            pltpu.make_async_copy(source, target, load_sem.at[number]).start()

    for number in range(4):
        load(number)

    def bytes_of(ref):
        return ref.dtype.itemsize * functools.reduce(lambda a, b: a * b, ref.shape)

    def span_of(total):
        if total < bytes_of(snd_v):
            return snd_v.at[:, pl.ds(0, total // snd_v.dtype.itemsize)]
        if total < bytes_of(table):
            return table.at[pl.ds(0, total // (2 * features))]
        return before.at[pl.ds(0, total // (4 * features))]

    def loaded(number):
        view = span_of(sum(bytes_of(target) for _, target in groups[number]))
        pltpu.make_async_copy(view, view, load_sem.at[number]).wait()

    def offset(slot):
        return slot // 3 - 1, slot % 3 - 1

    def place(slot):
        if slot in SIDES:
            return rows + B_SIDE * SIDES.index(slot)
        return corner_base + BLOCK * CORNERS.index(slot)

    def size_of(slot):
        return B_SIDE if slot in SIDES else B_CORNER

    def mesh_copy(slot):
        dlat, dlon = offset(slot)
        size = size_of(slot)
        return pltpu.make_async_remote_copy(
            src_ref=table.at[pl.ds(grid_rows + strip(slot) * B_SIDE, size)],
            dst_ref=edge_table.at[pl.ds(place(slot) - cut, size)],
            send_sem=send_sem.at[1 - dlat],
            recv_sem=recv_sem.at[1 + dlat],
            device_id=there(-dlat, -dlon),
            device_id_type=MESH,
        )

    def sum_copy(slot):
        dlat, dlon = offset(slot)
        size = size_of(slot)
        return pltpu.make_async_remote_copy(
            src_ref=put_sum.at[pl.ds(place(slot) - rows, size)],
            dst_ref=got_sum.at[pl.ds(place(slot) - rows, size)],
            send_sem=send_sem.at[1 + dlat],
            recv_sem=recv_sem.at[4 - dlat],
            device_id=there(dlat, dlon),
            device_id_type=MESH,
        )

    def settle(sems, first, chosen, times=1):
        for dlat in (-1, 1, 0):
            count = times * sum(size_of(s) for s in chosen if offset(s)[0] == dlat)
            if count:

                def body(dlat=dlat, count=count):
                    view = table.at[pl.ds(0, count)]
                    pltpu.make_async_copy(view, view, sems.at[first + 1 + dlat]).wait()

                guarded(dlat, body)

    def each(chosen, sign, action):
        for dlat in (-1, 0, 1):
            members = [s for s in chosen if offset(s)[0] == sign * dlat]
            if members:

                def body(members=members):
                    for s in members:
                        action(s)

                guarded(dlat, body)

    def send_sides():
        arrivals = 2 + (lat > 0).astype(jnp.int32) + (lat < n_lat - 1).astype(jnp.int32)
        pl.semaphore_wait(barrier, arrivals)
        for dlat in (-1, 1):

            def tell(dlat=dlat):
                pl.semaphore_signal(
                    ready_sem.at[0 if dlat > 0 else 1],
                    inc=1,
                    device_id=there(dlat, 0),
                    device_id_type=MESH,
                )

            guarded(dlat, tell)
        each(SIDES, -1, lambda s: mesh_copy(s).start())

    def send_corners(dlat):
        def go():
            pl.semaphore_wait(ready_sem.at[0 if dlat < 0 else 1], 1)
            for s in CORNERS:
                if offset(s)[0] == -dlat:
                    mesh_copy(s).start()

        guarded(dlat, go)

    step = min(CHUNK, edges)
    starts = list(range(0, edges, step))
    digits = grid_rows // DIGIT
    lane = lax.broadcasted_iota(jnp.int32, (step, LANES), 1).astype(F32)
    lanes = [(lane + float(LANES * h)).astype(BF16) for h in range(DIGIT // LANES)]

    loaded(0)
    senders = snd_v[...]
    upper = lax.shift_left(lax.shift_right_logical(senders, 8), 8)
    lower = (senders - upper).astype(F32).astype(BF16)
    upper = upper.astype(F32).astype(BF16)

    for start in starts:
        span = pl.ds(start, step)
        low_v[span, :] = down(lower[:, start : start + step], LANES)
        high_v[span, :] = down(upper[:, start : start + step], LANES)

    loaded(1)
    loaded(2)
    high, low = [part.astype(F32) for part in halves(w_edge_v[...])]
    bias_high, bias_low = [part.astype(F32) for part in halves(bias_v[...])]
    blank = jnp.zeros((BLOCK - B_CORNER, features), F32)
    last = jnp.concatenate(
        [bias_high, bias_low, jnp.zeros((B_CORNER - 2, features), F32)], 0
    )
    own = nn(mesh_v[...], w_mesh_v[...])
    table[grid_rows:, :] = (
        0.5
        * jnp.concatenate(
            [own, jnp.zeros((corner_base - rows, features), F32)]
            + [blank, high, blank, low, blank, high, blank, last],
            0,
        )
    ).astype(BF16)
    send_sides()
    send_corners(-1)
    loaded(3)
    load(4)
    table[:grid_rows, :] = (0.5 * nn(grid_v[...], w_grid_v[...])).astype(BF16)

    picks = rcv_v[...]
    shift, spot = 0, picks
    for s in range(9):
        base = (0 if s == 4 else place(s) - strip(s) * B_SIDE) - s * rows
        if s == 0:
            spot = spot + base
        else:
            spot = spot + jnp.where(picks >= s * rows, base - shift, 0)
        shift = base
    spot = spot.astype(F32).astype(BF16)
    high, low = [part.astype(F32) for part in halves(geo_v[...])]
    empty = jnp.zeros((BLOCK - B_CORNER, edges), F32)
    ones = jnp.concatenate([jnp.ones((2, edges), F32), jnp.zeros((2, edges), F32)], 0)
    tail = jnp.concatenate(
        [jnp.zeros((corner_base - cut, edges), F32)]
        + [empty, high, empty, high, empty, low, empty, ones],
        0,
    ).astype(BF16)
    for number, start in enumerate(starts):
        if number == UP_AT:
            send_corners(1)
        span = pl.ds(start, step)
        at = down(spot[:, start : start + step], LANES)
        tiles = []
        for q in range(digits):
            digit = (high_v[span, :] - float(DIGIT * q)) + low_v[span, :]
            tiles += [equal(digit, lanes[h]) for h in range(DIGIT // LANES)]
        for h in range(slots // LANES):
            found = equal(at, lanes[h])
            if h * LANES == cut:
                twice = found.astype(F8)
                picks_8[span, :] = jnp.concatenate([twice, twice], 1)
                found = found + jnp.transpose(tail[:, start : start + step])
            tiles.append(found)
        before[span, :] = nn(jnp.concatenate(tiles, 1), table[...])

    settle(recv_sem, 0, SIDES + CORNERS)

    arrived = edge_table[...].astype(F32)
    rough = arrived.astype(F8)
    fine = (arrived - rough.astype(F32)).astype(F8)
    split = jnp.concatenate([rough, fine], 0)
    parts = []
    for start in starts:
        span = pl.ds(start, step)
        half = before[span, :] + nn(picks_8[span, :], split)
        half = half.astype(BF16)
        parts.append(half + half * jnp.tanh(half))
    hidden = jnp.concatenate(parts, 0)

    def gathered(first, count):
        row = lax.broadcasted_iota(jnp.int32, (count, edges), 0) + first
        at = jnp.broadcast_to(spot, (count, edges))
        return nn(equal(row.astype(F32).astype(BF16), at), hidden)

    put_sum[...] = gathered(rows, slots - rows).astype(BF16)
    each(SENT, 1, lambda s: sum_copy(s).start())

    loaded(4)
    fold = nn(w_message_v[...], w_node_v[features:, :]).astype(BF16)
    high, low = halves(gathered(0, rows))
    node_v[...] = (
        nn(mesh_v[...], w_node_v[:features, :]) + nn(high, fold) + nn(low, fold)
    )
    weights = w_output_v[...].astype(F32)
    center = jnp.mean(weights, axis=-1, keepdims=True)
    w_center[...] = (weights - center).astype(BF16)

    def rows_of(ref, spans):
        return jnp.concatenate([ref[pl.ds(*span), :].astype(F32) for span in spans], 0)

    def finish(spans, extra=None):
        node = rows_of(node_v, spans)
        if extra is not None:
            node = node + nn(extra[...], fold)
        node_hidden = (node * jax.nn.sigmoid(node)).astype(BF16)
        centered = nn(node_hidden, w_center[...])
        row_var = jnp.mean(centered * centered, axis=-1, keepdims=True)
        normed = centered * lax.rsqrt(row_var + 1e-05) * gain_v[...] + nbias_v[...]
        result = rows_of(mesh_v, spans) + normed
        first = 0
        for start, count in spans:
            out_ref[0, 0, pl.ds(start, count), :] = result[first : first + count].astype(BF16)
            first += count

    at_sides = [(strip(s) * B_SIDE, B_SIDE) for s in SIDES]
    at_corners = [(strip(s) * B_SIDE, BLOCK) for s in CORNERS]
    between = [(strip(s) * B_SIDE + BLOCK, B_SIDE - BLOCK) for s in CORNERS]
    finish([(border, rows - border)] + between)
    settle(recv_sem, 3, SIDES + CORNERS)
    finish(at_sides + at_corners, got_sum)

    settle(send_sem, 0, SIDES + CORNERS, 2)


def local(n_lon, n_lat, *args):
    args = [a.reshape(1, -1) if a.ndim == 1 else a for a in args]
    grid_latent, mesh_latent, geometry, senders = args[:4]
    rows, features = mesh_latent.shape[2:]
    grid_rows = grid_latent.shape[2]
    edges = senders.shape[2]
    slots = rows + 4 * B_SIDE + 4 * BLOCK
    cut = rows // LANES * LANES
    loads = []
    for number, a in enumerate(args):
        shape = a.shape[2:] if number < 3 else a.shape[1:] if number < 5 else a.shape
        loads.append(pltpu.VMEM(shape, a.dtype))
    return pl.pallas_call(
        functools.partial(kernel, n_lon, n_lat),
        out_shape=pltpu.VMEM(mesh_latent.shape, BF16),
        in_specs=[pl.BlockSpec(memory_space=pl.ANY)] * len(args),
        out_specs=pl.BlockSpec(memory_space=pltpu.VMEM),
        scratch_shapes=loads
        + [
            pltpu.VMEM((grid_rows + slots, features), BF16),
            pltpu.VMEM((slots - cut, features), BF16),
            pltpu.VMEM((edges, LANES), BF16),
            pltpu.VMEM((edges, LANES), BF16),
            pltpu.VMEM((edges, 2 * LANES), F8),
            pltpu.VMEM((edges, features), F32),
            pltpu.VMEM((slots - rows, features), BF16),
            pltpu.VMEM((slots - rows, features), BF16),
            pltpu.VMEM((features, features), BF16),
            pltpu.VMEM((rows, features), F32),
            pltpu.SemaphoreType.DMA((5,)),
            pltpu.SemaphoreType.DMA((3,)),
            pltpu.SemaphoreType.DMA((6,)),
            pltpu.SemaphoreType.REGULAR((2,)),
        ],
        compiler_params=pltpu.CompilerParams(
            collective_id=0, has_side_effects=True, vmem_limit_bytes=56 * 1024 * 1024
        ),
    )(*args)


def solution(mesh):
    return jax.shard_map(
        functools.partial(local, mesh.shape["lon"], mesh.shape["lat"]),
        mesh=mesh,
        in_specs=(
            P("lat", "lon", None, None),
            P("lat", "lon", None, None),
            P("lat", "lon", None, None),
            P("lat", "lon", None),
            P("lat", "lon", None),
            P(),
            P(),
            P(),
            P(),
            P(),
            P(),
            P(),
            P(),
            P(),
        ),
        out_specs=P("lat", "lon", None, None),
        check_vma=False,
    )
```

```python
import functools

import jax
import jax.numpy as jnp
from jax import lax
from jax.experimental import pallas as pl
from jax.experimental.pallas import tpu as pltpu
from jax.sharding import PartitionSpec as P

B_SIDE = 16
B_CORNER = 4
BLOCK = 8
LANES = 128
DIGIT = 256
CHUNK = 256
UP_AT = 1
BURSTS = (1, 2, 3, 2)
LAG = 1
MESH = pl.DeviceIdType.MESH

BF16 = jnp.bfloat16
F32 = jnp.float32
F8 = jnp.float8_e4m3fn

SIDES = (1, 3, 5, 7)
CORNERS = (0, 2, 6, 8)
SENT = (2, 1, 0, 3, 5, 7, 8, 6)


def strip(slot):
    return slot if slot < 4 else slot - 1


def nn(a, b):
    return jnp.dot(a, b, preferred_element_type=F32)


def halves(x):
    high = x.astype(BF16)
    return high, (x - high.astype(F32)).astype(BF16)


def down(row, count):
    return jnp.transpose(jnp.broadcast_to(row, (count, row.shape[1])))


def equal(a, b):
    one = jnp.ones(a.shape, BF16)
    return jnp.where(a == b, one, jnp.zeros_like(one))


def kernel(
    n_lon,
    n_lat,
    grid_h,
    mesh_h,
    geo_h,
    snd_h,
    rcv_h,
    w_grid_h,
    w_mesh_h,
    w_edge_h,
    bias_h,
    w_message_h,
    w_node_h,
    w_output_h,
    gain_h,
    nbias_h,
    out_ref,
    grid_v,
    mesh_v,
    geo_v,
    snd_v,
    rcv_v,
    w_grid_v,
    w_mesh_v,
    w_edge_v,
    bias_v,
    w_message_v,
    w_node_v,
    w_output_v,
    gain_v,
    nbias_v,
    table,
    edge_table,
    low_v,
    high_v,
    picks_8,
    before,
    put_sum,
    got_sum,
    w_center,
    node_v,
    load_sem,
    send_sem,
    recv_sem,
    ready_sem,
):
    lon = lax.axis_index("lon")
    lat = lax.axis_index("lat")
    rows, features = mesh_v.shape
    grid_rows = grid_v.shape[0]
    edges = snd_v.shape[1]
    corner_base = rows + 4 * B_SIDE
    slots = corner_base + 4 * BLOCK
    cut = rows // LANES * LANES
    border = 8 * B_SIDE

    def there(dlat, dlon):
        return {
            "lat": lat + dlat,
            "lon": lax.rem(lon + dlon + n_lon, n_lon),
        }

    def guarded(dlat, body):
        if dlat == 0:
            body()
        else:
            pl.when(lat > 0 if dlat < 0 else lat < n_lat - 1)(body)

    edge_table[...] = jnp.zeros(edge_table.shape, BF16)
    got_sum[...] = jnp.zeros(got_sum.shape, BF16)

    barrier = pltpu.get_barrier_semaphore()

    def greet(dlat, dlon):
        pl.semaphore_signal(barrier, inc=1, device_id=there(dlat, dlon), device_id_type=MESH)

    greet(0, -1)
    greet(0, 1)
    guarded(-1, lambda: greet(-1, 0))
    guarded(1, lambda: greet(1, 0))

    groups = [
        [(snd_h.at[0], snd_v)],
        [
            (mesh_h.at[0, 0], mesh_v),
            (w_mesh_h, w_mesh_v),
            (w_edge_h, w_edge_v),
            (rcv_h.at[0], rcv_v),
            (geo_h.at[0, 0], geo_v),
        ],
        [(bias_h, bias_v), (gain_h, gain_v), (nbias_h, nbias_v)],
        [(w_grid_h, w_grid_v), (grid_h.at[0, 0], grid_v)],
        [(w_message_h, w_message_v), (w_node_h, w_node_v), (w_output_h, w_output_v)],
    ]

    def load(number):
        for source, target in groups[number]:
            pltpu.make_async_copy(source, target, load_sem.at[number]).start()

    for number in range(4):
        load(number)

    def bytes_of(ref):
        return ref.dtype.itemsize * functools.reduce(lambda a, b: a * b, ref.shape)

    def span_of(total):
        if total < bytes_of(snd_v):
            return snd_v.at[:, pl.ds(0, total // snd_v.dtype.itemsize)]
        if total < bytes_of(table):
            return table.at[pl.ds(0, total // (2 * features))]
        return before.at[pl.ds(0, total // (4 * features))]

    def loaded(number):
        view = span_of(sum(bytes_of(target) for _, target in groups[number]))
        pltpu.make_async_copy(view, view, load_sem.at[number]).wait()

    def offset(slot):
        return slot // 3 - 1, slot % 3 - 1

    def place(slot):
        if slot in SIDES:
            return rows + B_SIDE * SIDES.index(slot)
        return corner_base + BLOCK * CORNERS.index(slot)

    def size_of(slot):
        return B_SIDE if slot in SIDES else B_CORNER

    def mesh_copy(slot):
        dlat, dlon = offset(slot)
        size = size_of(slot)
        return pltpu.make_async_remote_copy(
            src_ref=table.at[pl.ds(grid_rows + strip(slot) * B_SIDE, size)],
            dst_ref=edge_table.at[pl.ds(place(slot) - cut, size)],
            send_sem=send_sem.at[1 - dlat],
            recv_sem=recv_sem.at[1 + dlat],
            device_id=there(-dlat, -dlon),
            device_id_type=MESH,
        )

    def sum_copy(slot):
        dlat, dlon = offset(slot)
        size = size_of(slot)
        return pltpu.make_async_remote_copy(
            src_ref=put_sum.at[pl.ds(place(slot) - rows, size)],
            dst_ref=got_sum.at[pl.ds(place(slot) - rows, size)],
            send_sem=send_sem.at[1 + dlat],
            recv_sem=recv_sem.at[4 - dlat],
            device_id=there(dlat, dlon),
            device_id_type=MESH,
        )

    def settle(sems, first, chosen, times=1):
        for dlat in (-1, 1, 0):
            count = times * sum(size_of(s) for s in chosen if offset(s)[0] == dlat)
            if count:

                def body(dlat=dlat, count=count):
                    view = table.at[pl.ds(0, count)]
                    pltpu.make_async_copy(view, view, sems.at[first + 1 + dlat]).wait()

                guarded(dlat, body)

    def each(chosen, sign, action):
        for dlat in (-1, 0, 1):
            members = [s for s in chosen if offset(s)[0] == sign * dlat]
            if members:

                def body(members=members):
                    for s in members:
                        action(s)

                guarded(dlat, body)

    def send_sides():
        arrivals = 2 + (lat > 0).astype(jnp.int32) + (lat < n_lat - 1).astype(jnp.int32)
        pl.semaphore_wait(barrier, arrivals)
        for dlat in (-1, 1):

            def tell(dlat=dlat):
                pl.semaphore_signal(
                    ready_sem.at[0 if dlat > 0 else 1],
                    inc=1,
                    device_id=there(dlat, 0),
                    device_id_type=MESH,
                )

            guarded(dlat, tell)
        each(SIDES, -1, lambda s: mesh_copy(s).start())

    def send_corners(dlat):
        def go():
            pl.semaphore_wait(ready_sem.at[0 if dlat < 0 else 1], 1)
            for s in reversed(CORNERS):
                if offset(s)[0] == -dlat:
                    mesh_copy(s).start()

        guarded(dlat, go)

    step = min(CHUNK, edges)
    starts = list(range(0, edges, step))
    digits = grid_rows // DIGIT
    lane = lax.broadcasted_iota(jnp.int32, (step, LANES), 1).astype(F32)
    lanes = [(lane + float(LANES * h)).astype(BF16) for h in range(DIGIT // LANES)]

    loaded(0)
    senders = snd_v[...]
    upper = lax.shift_left(lax.shift_right_logical(senders, 8), 8)
    lower = (senders - upper).astype(F32).astype(BF16)
    upper = upper.astype(F32).astype(BF16)

    for start in starts:
        span = pl.ds(start, step)
        low_v[span, :] = down(lower[:, start : start + step], LANES)
        high_v[span, :] = down(upper[:, start : start + step], LANES)

    loaded(1)
    loaded(2)
    high, low = [part.astype(F32) for part in halves(w_edge_v[...])]
    bias_high, bias_low = [part.astype(F32) for part in halves(bias_v[...])]
    blank = jnp.zeros((BLOCK - B_CORNER, features), F32)
    last = jnp.concatenate(
        [bias_high, bias_low, jnp.zeros((B_CORNER - 2, features), F32)], 0
    )
    own = nn(mesh_v[...], w_mesh_v[...])
    table[grid_rows:, :] = (
        0.5
        * jnp.concatenate(
            [own, jnp.zeros((corner_base - rows, features), F32)]
            + [blank, high, blank, low, blank, high, blank, last],
            0,
        )
    ).astype(BF16)
    send_sides()
    send_corners(-1)
    loaded(3)
    load(4)
    table[:grid_rows, :] = (0.5 * nn(grid_v[...], w_grid_v[...])).astype(BF16)

    picks = rcv_v[...]
    shift, spot = 0, picks
    for s in range(9):
        base = (0 if s == 4 else place(s) - strip(s) * B_SIDE) - s * rows
        if s == 0:
            spot = spot + base
        else:
            spot = spot + jnp.where(picks >= s * rows, base - shift, 0)
        shift = base
    spot = spot.astype(F32).astype(BF16)
    high, low = [part.astype(F32) for part in halves(geo_v[...])]
    empty = jnp.zeros((BLOCK - B_CORNER, edges), F32)
    ones = jnp.concatenate([jnp.ones((2, edges), F32), jnp.zeros((2, edges), F32)], 0)
    tail = jnp.concatenate(
        [jnp.zeros((corner_base - cut, edges), F32)]
        + [empty, high, empty, high, empty, low, empty, ones],
        0,
    ).astype(BF16)
    for number, start in enumerate(starts):
        if number == UP_AT:
            send_corners(1)
        span = pl.ds(start, step)
        at = down(spot[:, start : start + step], LANES)
        tiles = []
        for q in range(digits):
            digit = (high_v[span, :] - float(DIGIT * q)) + low_v[span, :]
            tiles += [equal(digit, lanes[h]) for h in range(DIGIT // LANES)]
        for h in range(slots // LANES):
            found = equal(at, lanes[h])
            if h * LANES == cut:
                twice = found.astype(F8)
                picks_8[span, :] = jnp.concatenate([twice, twice], 1)
                found = found + jnp.transpose(tail[:, start : start + step])
            tiles.append(found)
        before[span, :] = nn(jnp.concatenate(tiles, 1), table[...])

    settle(recv_sem, 0, SIDES + CORNERS)

    arrived = edge_table[...].astype(F32)
    rough = arrived.astype(F8)
    fine = (arrived - rough.astype(F32)).astype(F8)
    split = jnp.concatenate([rough, fine], 0)
    def gathered(first, count, begin, hidden):
        width = hidden.shape[0]
        row = lax.broadcasted_iota(jnp.int32, (count, width), 0) + first
        at = jnp.broadcast_to(spot[:, begin : begin + width], (count, width))
        return nn(equal(row.astype(F32).astype(BF16), at), hidden)

    unit = edges // sum(BURSTS)
    sizes = [unit * count for count in BURSTS]
    begins = [sum(sizes[:number]) for number in range(len(sizes))]
    halves_of, parts, summed = [], [], None
    for number in range(len(sizes) + LAG):
        if number < len(sizes):
            span = pl.ds(begins[number], sizes[number])
            half = before[span, :] + nn(picks_8[span, :], split)
            halves_of.append(half.astype(BF16))
        if 1 <= number <= len(sizes):
            half = halves_of[number - 1]
            parts.append(half + half * jnp.tanh(half))
        if number >= LAG:
            done = number - LAG
            added = gathered(rows, slots - rows, begins[done], parts[done])
            summed = added if summed is None else summed + added

    put_sum[...] = summed.astype(BF16)
    each(SENT, 1, lambda s: sum_copy(s).start())

    loaded(4)
    fold = nn(w_message_v[...], w_node_v[features:, :]).astype(BF16)
    high, low = halves(gathered(0, rows, 0, jnp.concatenate(parts, 0)))
    node_v[...] = (
        nn(mesh_v[...], w_node_v[:features, :]) + nn(high, fold) + nn(low, fold)
    )
    weights = w_output_v[...].astype(F32)
    center = jnp.mean(weights, axis=-1, keepdims=True)
    w_center[...] = (weights - center).astype(BF16)

    def rows_of(ref, spans):
        return jnp.concatenate([ref[pl.ds(*span), :].astype(F32) for span in spans], 0)

    def finish(spans, extra=None):
        node = rows_of(node_v, spans)
        if extra is not None:
            node = node + nn(extra[...], fold)
        node_hidden = (node * jax.nn.sigmoid(node)).astype(BF16)
        centered = nn(node_hidden, w_center[...])
        row_var = jnp.mean(centered * centered, axis=-1, keepdims=True)
        normed = centered * lax.rsqrt(row_var + 1e-05) * gain_v[...] + nbias_v[...]
        result = rows_of(mesh_v, spans) + normed
        first = 0
        for start, count in spans:
            out_ref[0, 0, pl.ds(start, count), :] = result[first : first + count].astype(BF16)
            first += count

    at_sides = [(strip(s) * B_SIDE, B_SIDE) for s in SIDES]
    at_corners = [(strip(s) * B_SIDE, BLOCK) for s in CORNERS]
    between = [(strip(s) * B_SIDE + BLOCK, B_SIDE - BLOCK) for s in CORNERS]
    finish([(border, rows - border)] + between)
    settle(recv_sem, 3, SIDES + CORNERS)
    finish(at_sides + at_corners, got_sum)

    settle(send_sem, 0, SIDES + CORNERS, 2)


def local(n_lon, n_lat, *args):
    args = [a.reshape(1, -1) if a.ndim == 1 else a for a in args]
    grid_latent, mesh_latent, geometry, senders = args[:4]
    rows, features = mesh_latent.shape[2:]
    grid_rows = grid_latent.shape[2]
    edges = senders.shape[2]
    slots = rows + 4 * B_SIDE + 4 * BLOCK
    cut = rows // LANES * LANES
    loads = []
    for number, a in enumerate(args):
        shape = a.shape[2:] if number < 3 else a.shape[1:] if number < 5 else a.shape
        loads.append(pltpu.VMEM(shape, a.dtype))
    return pl.pallas_call(
        functools.partial(kernel, n_lon, n_lat),
        out_shape=pltpu.VMEM(mesh_latent.shape, BF16),
        in_specs=[pl.BlockSpec(memory_space=pl.ANY)] * len(args),
        out_specs=pl.BlockSpec(memory_space=pltpu.VMEM),
        scratch_shapes=loads
        + [
            pltpu.VMEM((grid_rows + slots, features), BF16),
            pltpu.VMEM((slots - cut, features), BF16),
            pltpu.VMEM((edges, LANES), BF16),
            pltpu.VMEM((edges, LANES), BF16),
            pltpu.VMEM((edges, 2 * LANES), F8),
            pltpu.VMEM((edges, features), F32),
            pltpu.VMEM((slots - rows, features), BF16),
            pltpu.VMEM((slots - rows, features), BF16),
            pltpu.VMEM((features, features), BF16),
            pltpu.VMEM((rows, features), F32),
            pltpu.SemaphoreType.DMA((5,)),
            pltpu.SemaphoreType.DMA((3,)),
            pltpu.SemaphoreType.DMA((6,)),
            pltpu.SemaphoreType.REGULAR((2,)),
        ],
        compiler_params=pltpu.CompilerParams(
            collective_id=0, has_side_effects=True, vmem_limit_bytes=56 * 1024 * 1024
        ),
    )(*args)


def solution(mesh):
    return jax.shard_map(
        functools.partial(local, mesh.shape["lon"], mesh.shape["lat"]),
        mesh=mesh,
        in_specs=(
            P("lat", "lon", None, None),
            P("lat", "lon", None, None),
            P("lat", "lon", None, None),
            P("lat", "lon", None),
            P("lat", "lon", None),
            P(),
            P(),
            P(),
            P(),
            P(),
            P(),
            P(),
            P(),
            P(),
        ),
        out_specs=P("lat", "lon", None, None),
        check_vma=False,
    )
```

```python
import functools

import jax
import jax.numpy as jnp
from jax import lax
from jax.experimental import pallas as pl
from jax.experimental.pallas import tpu as pltpu
from jax.sharding import PartitionSpec as P

B_SIDE = 16
B_CORNER = 4
BLOCK = 8
LANES = 128
DIGIT = 256
CHUNK = 256
UP_AT = 1
BURSTS = (1, 2, 3, 2)
LAG = 1
MESH = pl.DeviceIdType.MESH

BF16 = jnp.bfloat16
F32 = jnp.float32
F8 = jnp.float8_e4m3fn

SIDES = (1, 3, 5, 7)
CORNERS = (0, 2, 6, 8)
SENT = (2, 1, 0, 3, 5, 7, 8, 6)


def strip(slot):
    return slot if slot < 4 else slot - 1


def nn(a, b):
    return jnp.dot(a, b, preferred_element_type=F32)


def halves(x):
    high = x.astype(BF16)
    return high, (x - high.astype(F32)).astype(BF16)


def down(row, count):
    return jnp.transpose(jnp.broadcast_to(row, (count, row.shape[1])))


def equal(a, b):
    one = jnp.ones(a.shape, BF16)
    return jnp.where(a == b, one, jnp.zeros_like(one))


def kernel(
    n_lon,
    n_lat,
    grid_h,
    mesh_h,
    geo_h,
    snd_h,
    rcv_h,
    w_grid_h,
    w_mesh_h,
    w_edge_h,
    bias_h,
    w_message_h,
    w_node_h,
    w_output_h,
    gain_h,
    nbias_h,
    out_ref,
    grid_v,
    mesh_v,
    geo_v,
    snd_v,
    rcv_v,
    w_grid_v,
    w_mesh_v,
    w_edge_v,
    bias_v,
    w_message_v,
    w_node_v,
    w_output_v,
    gain_v,
    nbias_v,
    table,
    edge_table,
    low_v,
    high_v,
    picks_8,
    before,
    put_sum,
    got_sum,
    w_center,
    node_v,
    ruler,
    load_sem,
    strip_sem,
    ready_sem,
):
    lon = lax.axis_index("lon")
    lat = lax.axis_index("lat")
    rows, features = mesh_v.shape
    grid_rows = grid_v.shape[0]
    edges = snd_v.shape[1]
    corner_base = rows + 4 * B_SIDE
    slots = corner_base + 4 * BLOCK
    cut = rows // LANES * LANES
    border = 8 * B_SIDE

    def there(dlat, dlon):
        return {
            "lat": lat + dlat,
            "lon": lax.rem(lon + dlon + n_lon, n_lon),
        }

    def guarded(dlat, body):
        if dlat == 0:
            body()
        else:
            pl.when(lat > 0 if dlat < 0 else lat < n_lat - 1)(body)

    edge_table[...] = jnp.zeros(edge_table.shape, BF16)
    got_sum[...] = jnp.zeros(got_sum.shape, BF16)

    barrier = pltpu.get_barrier_semaphore()

    def greet(dlat, dlon):
        pl.semaphore_signal(barrier, inc=1, device_id=there(dlat, dlon), device_id_type=MESH)

    greet(0, -1)
    greet(0, 1)
    guarded(-1, lambda: greet(-1, 0))
    guarded(1, lambda: greet(1, 0))

    groups = [
        [(snd_h.at[0], snd_v)],
        [
            (mesh_h.at[0, 0], mesh_v),
            (w_mesh_h, w_mesh_v),
            (w_edge_h, w_edge_v),
            (rcv_h.at[0], rcv_v),
            (geo_h.at[0, 0], geo_v),
            (bias_h, bias_v),
            (gain_h, gain_v),
            (nbias_h, nbias_v),
        ],
        [(w_grid_h, w_grid_v), (grid_h.at[0, 0], grid_v)],
        [(w_message_h, w_message_v), (w_node_h, w_node_v), (w_output_h, w_output_v)],
    ]

    def load(number):
        for source, target in groups[number]:
            pltpu.make_async_copy(source, target, load_sem.at[number % 3]).start()

    for number in range(3):
        load(number)

    def bytes_of(ref):
        return ref.dtype.itemsize * functools.reduce(lambda a, b: a * b, ref.shape)

    def await_bytes(total, sem):
        view = ruler.at[:, pl.ds(0, total // ruler.dtype.itemsize)]
        pltpu.make_async_copy(view, view, sem).wait()

    def loaded(number):
        total = sum(bytes_of(target) for _, target in groups[number])
        await_bytes(total, load_sem.at[number % 3])

    def offset(slot):
        return slot // 3 - 1, slot % 3 - 1

    def place(slot):
        if slot in SIDES:
            return rows + B_SIDE * SIDES.index(slot)
        return corner_base + BLOCK * CORNERS.index(slot)

    def size_of(slot):
        return B_SIDE if slot in SIDES else B_CORNER

    def mesh_copy(slot):
        dlat, dlon = offset(slot)
        size = size_of(slot)
        return pltpu.make_async_remote_copy(
            src_ref=table.at[pl.ds(grid_rows + strip(slot) * B_SIDE, size)],
            dst_ref=edge_table.at[pl.ds(place(slot) - cut, size)],
            send_sem=strip_sem.at[0],
            recv_sem=strip_sem.at[1],
            device_id=there(-dlat, -dlon),
            device_id_type=MESH,
        )

    def sum_copy(slot):
        dlat, dlon = offset(slot)
        size = size_of(slot)
        return pltpu.make_async_remote_copy(
            src_ref=put_sum.at[pl.ds(place(slot) - rows, size)],
            dst_ref=got_sum.at[pl.ds(place(slot) - rows, size)],
            send_sem=strip_sem.at[0],
            recv_sem=strip_sem.at[2],
            device_id=there(dlat, dlon),
            device_id_type=MESH,
        )

    bands = (lat > 0).astype(jnp.int32) + (lat < n_lat - 1).astype(jnp.int32)

    def settle(sem, times):
        for count in range(3):

            def body(count=count):
                lines = 2 * B_SIDE + count * (B_SIDE + 2 * B_CORNER)
                await_bytes(times * lines * features * 2, sem)

            pl.when(bands == count)(body)

    def each(chosen, sign, action):
        for dlat in (-1, 0, 1):
            members = [s for s in chosen if offset(s)[0] == sign * dlat]
            if members:

                def body(members=members):
                    for s in members:
                        action(s)

                guarded(dlat, body)

    def send_sides():
        pl.semaphore_wait(barrier, 2 + bands)
        for dlat in (-1, 1):

            def tell(dlat=dlat):
                pl.semaphore_signal(
                    ready_sem.at[0 if dlat > 0 else 1],
                    inc=1,
                    device_id=there(dlat, 0),
                    device_id_type=MESH,
                )

            guarded(dlat, tell)
        each(SIDES, -1, lambda s: mesh_copy(s).start())

    def send_corners(dlat):
        def go():
            pl.semaphore_wait(ready_sem.at[0 if dlat < 0 else 1], 1)
            for s in reversed(CORNERS):
                if offset(s)[0] == -dlat:
                    mesh_copy(s).start()

        guarded(dlat, go)

    step = min(CHUNK, edges)
    starts = list(range(0, edges, step))
    digits = grid_rows // DIGIT
    lane = lax.broadcasted_iota(jnp.int32, (step, LANES), 1).astype(F32)
    lanes = [(lane + float(LANES * h)).astype(BF16) for h in range(DIGIT // LANES)]

    loaded(0)
    senders = snd_v[...]
    upper = lax.shift_left(lax.shift_right_logical(senders, 8), 8)
    lower = (senders - upper).astype(F32).astype(BF16)
    upper = upper.astype(F32).astype(BF16)

    for start in starts:
        span = pl.ds(start, step)
        low_v[span, :] = down(lower[:, start : start + step], LANES)
        high_v[span, :] = down(upper[:, start : start + step], LANES)

    loaded(1)
    high, low = [part.astype(F32) for part in halves(w_edge_v[...])]
    bias_high, bias_low = [part.astype(F32) for part in halves(bias_v[...])]
    blank = jnp.zeros((BLOCK - B_CORNER, features), F32)
    last = jnp.concatenate(
        [bias_high, bias_low, jnp.zeros((B_CORNER - 2, features), F32)], 0
    )
    own = nn(mesh_v[...], w_mesh_v[...])
    table[grid_rows:, :] = (
        0.5
        * jnp.concatenate(
            [own, jnp.zeros((corner_base - rows, features), F32)]
            + [blank, high, blank, low, blank, high, blank, last],
            0,
        )
    ).astype(BF16)
    send_sides()
    send_corners(-1)
    loaded(2)
    load(3)
    table[:grid_rows, :] = (0.5 * nn(grid_v[...], w_grid_v[...])).astype(BF16)

    picks = rcv_v[...]
    shift, spot = 0, picks
    for s in range(9):
        base = (0 if s == 4 else place(s) - strip(s) * B_SIDE) - s * rows
        if s == 0:
            spot = spot + base
        else:
            spot = spot + jnp.where(picks >= s * rows, base - shift, 0)
        shift = base
    spot = spot.astype(F32).astype(BF16)
    high, low = [part.astype(F32) for part in halves(geo_v[...])]
    empty = jnp.zeros((BLOCK - B_CORNER, edges), F32)
    ones = jnp.concatenate([jnp.ones((2, edges), F32), jnp.zeros((2, edges), F32)], 0)
    tail = jnp.concatenate(
        [jnp.zeros((corner_base - cut, edges), F32)]
        + [empty, high, empty, high, empty, low, empty, ones],
        0,
    ).astype(BF16)
    for number, start in enumerate(starts):
        if number == UP_AT:
            send_corners(1)
        span = pl.ds(start, step)
        at = down(spot[:, start : start + step], LANES)
        tiles = []
        for q in range(digits):
            digit = (high_v[span, :] - float(DIGIT * q)) + low_v[span, :]
            tiles += [equal(digit, lanes[h]) for h in range(DIGIT // LANES)]
        for h in range(slots // LANES):
            found = equal(at, lanes[h])
            if h * LANES == cut:
                twice = found.astype(F8)
                picks_8[span, :] = jnp.concatenate([twice, twice], 1)
                found = found + jnp.transpose(tail[:, start : start + step])
            tiles.append(found)
        before[span, :] = nn(jnp.concatenate(tiles, 1), table[...])

    settle(strip_sem.at[1], 1)

    arrived = edge_table[...].astype(F32)
    rough = arrived.astype(F8)
    fine = (arrived - rough.astype(F32)).astype(F8)
    split = jnp.concatenate([rough, fine], 0)
    def gathered(first, count, begin, hidden):
        width = hidden.shape[0]
        row = lax.broadcasted_iota(jnp.int32, (count, width), 0) + first
        at = jnp.broadcast_to(spot[:, begin : begin + width], (count, width))
        return nn(equal(row.astype(F32).astype(BF16), at), hidden)

    unit = edges // sum(BURSTS)
    sizes = [unit * count for count in BURSTS]
    begins = [sum(sizes[:number]) for number in range(len(sizes))]
    halves_of, parts, summed = [], [], None
    for number in range(len(sizes) + LAG):
        if number < len(sizes):
            span = pl.ds(begins[number], sizes[number])
            half = before[span, :] + nn(picks_8[span, :], split)
            halves_of.append(half.astype(BF16))
        if 1 <= number <= len(sizes):
            half = halves_of[number - 1]
            parts.append(half + half * jnp.tanh(half))
        if number >= LAG:
            done = number - LAG
            added = gathered(rows, slots - rows, begins[done], parts[done])
            summed = added if summed is None else summed + added

    put_sum[...] = summed.astype(BF16)
    each(SENT, 1, lambda s: sum_copy(s).start())

    loaded(3)
    fold = nn(w_message_v[...], w_node_v[features:, :]).astype(BF16)
    high, low = halves(gathered(0, rows, 0, jnp.concatenate(parts, 0)))
    node_v[...] = (
        nn(mesh_v[...], w_node_v[:features, :]) + nn(high, fold) + nn(low, fold)
    )
    weights = w_output_v[...].astype(F32)
    center = jnp.mean(weights, axis=-1, keepdims=True)
    w_center[...] = (weights - center).astype(BF16)

    def rows_of(ref, spans):
        return jnp.concatenate([ref[pl.ds(*span), :].astype(F32) for span in spans], 0)

    def finish(spans, extra=None):
        node = rows_of(node_v, spans)
        if extra is not None:
            node = node + nn(extra[...], fold)
        node_hidden = (node * jax.nn.sigmoid(node)).astype(BF16)
        centered = nn(node_hidden, w_center[...])
        row_var = jnp.mean(centered * centered, axis=-1, keepdims=True)
        normed = centered * lax.rsqrt(row_var + 1e-05) * gain_v[...] + nbias_v[...]
        result = rows_of(mesh_v, spans) + normed
        first = 0
        for start, count in spans:
            out_ref[0, 0, pl.ds(start, count), :] = result[first : first + count].astype(BF16)
            first += count

    at_sides = [(strip(s) * B_SIDE, B_SIDE) for s in SIDES]
    at_corners = [(strip(s) * B_SIDE, BLOCK) for s in CORNERS]
    between = [(strip(s) * B_SIDE + BLOCK, B_SIDE - BLOCK) for s in CORNERS]
    finish([(border, rows - border)] + between)
    settle(strip_sem.at[2], 1)
    finish(at_sides + at_corners, got_sum)

    settle(strip_sem.at[0], 2)


def local(n_lon, n_lat, *args):
    args = [a.reshape(1, -1) if a.ndim == 1 else a for a in args]
    grid_latent, mesh_latent, geometry, senders = args[:4]
    rows, features = mesh_latent.shape[2:]
    grid_rows = grid_latent.shape[2]
    edges = senders.shape[2]
    slots = rows + 4 * B_SIDE + 4 * BLOCK
    cut = rows // LANES * LANES
    ruler = sum(a.size * a.dtype.itemsize for a in args[9:12]) // 4
    loads = []
    for number, a in enumerate(args):
        shape = a.shape[2:] if number < 3 else a.shape[1:] if number < 5 else a.shape
        loads.append(pltpu.VMEM(shape, a.dtype))
    return pl.pallas_call(
        functools.partial(kernel, n_lon, n_lat),
        out_shape=pltpu.VMEM(mesh_latent.shape, BF16),
        in_specs=[pl.BlockSpec(memory_space=pl.ANY)] * len(args),
        out_specs=pl.BlockSpec(memory_space=pltpu.VMEM),
        scratch_shapes=loads
        + [
            pltpu.VMEM((grid_rows + slots, features), BF16),
            pltpu.VMEM((slots - cut, features), BF16),
            pltpu.VMEM((edges, LANES), BF16),
            pltpu.VMEM((edges, LANES), BF16),
            pltpu.VMEM((edges, 2 * LANES), F8),
            pltpu.VMEM((edges, features), F32),
            pltpu.VMEM((slots - rows, features), BF16),
            pltpu.VMEM((slots - rows, features), BF16),
            pltpu.VMEM((features, features), BF16),
            pltpu.VMEM((rows, features), F32),
            pltpu.VMEM((1, ruler), jnp.int32),
            pltpu.SemaphoreType.DMA((3,)),
            pltpu.SemaphoreType.DMA((3,)),
            pltpu.SemaphoreType.REGULAR((2,)),
        ],
        compiler_params=pltpu.CompilerParams(
            collective_id=0, has_side_effects=True, vmem_limit_bytes=56 * 1024 * 1024
        ),
    )(*args)


def solution(mesh):
    return jax.shard_map(
        functools.partial(local, mesh.shape["lon"], mesh.shape["lat"]),
        mesh=mesh,
        in_specs=(
            P("lat", "lon", None, None),
            P("lat", "lon", None, None),
            P("lat", "lon", None, None),
            P("lat", "lon", None),
            P("lat", "lon", None),
            P(),
            P(),
            P(),
            P(),
            P(),
            P(),
            P(),
            P(),
            P(),
        ),
        out_specs=P("lat", "lon", None, None),
        check_vma=False,
    )
```

```python
import functools

import jax
import jax.numpy as jnp
from jax import lax
from jax.experimental import pallas as pl
from jax.experimental.pallas import tpu as pltpu
from jax.sharding import PartitionSpec as P

B_SIDE = 16
B_CORNER = 4
BLOCK = 8
LANES = 128
DIGIT = 256
CHUNK = 256
UP_AT = 1
BURSTS = (1, 1, 2, 2, 2)
LAG = 1
MESH = pl.DeviceIdType.MESH

BF16 = jnp.bfloat16
F32 = jnp.float32
F8 = jnp.float8_e4m3fn

SIDES = (1, 3, 5, 7)
CORNERS = (0, 2, 6, 8)
SENT = (2, 1, 0, 3, 5, 7, 8, 6)


def strip(slot):
    return slot if slot < 4 else slot - 1


def nn(a, b):
    return jnp.dot(a, b, preferred_element_type=F32)


def halves(x):
    high = x.astype(BF16)
    return high, (x - high.astype(F32)).astype(BF16)


def down(row, count):
    return jnp.transpose(jnp.broadcast_to(row, (count, row.shape[1])))


def equal(a, b):
    one = jnp.ones(a.shape, BF16)
    return jnp.where(a == b, one, jnp.zeros_like(one))


def kernel(
    n_lon,
    n_lat,
    grid_h,
    mesh_h,
    geo_h,
    snd_h,
    rcv_h,
    w_grid_h,
    w_mesh_h,
    w_edge_h,
    bias_h,
    w_message_h,
    w_node_h,
    w_output_h,
    gain_h,
    nbias_h,
    out_ref,
    grid_v,
    mesh_v,
    geo_v,
    snd_v,
    rcv_v,
    w_grid_v,
    w_mesh_v,
    w_edge_v,
    bias_v,
    w_message_v,
    w_node_v,
    w_output_v,
    gain_v,
    nbias_v,
    table,
    edge_table,
    low_v,
    high_v,
    picks_8,
    before,
    put_sum,
    got_sum,
    w_center,
    node_v,
    ruler,
    load_sem,
    strip_sem,
    ready_sem,
):
    lon = lax.axis_index("lon")
    lat = lax.axis_index("lat")
    rows, features = mesh_v.shape
    grid_rows = grid_v.shape[0]
    edges = snd_v.shape[1]
    corner_base = rows + 4 * B_SIDE
    slots = corner_base + 4 * BLOCK
    cut = rows // LANES * LANES
    border = 8 * B_SIDE

    def there(dlat, dlon):
        return {
            "lat": lat + dlat,
            "lon": lax.rem(lon + dlon + n_lon, n_lon),
        }

    def guarded(dlat, body):
        if dlat == 0:
            body()
        else:
            pl.when(lat > 0 if dlat < 0 else lat < n_lat - 1)(body)

    edge_table[...] = jnp.zeros(edge_table.shape, BF16)
    got_sum[...] = jnp.zeros(got_sum.shape, BF16)

    barrier = pltpu.get_barrier_semaphore()

    def greet(dlat, dlon):
        pl.semaphore_signal(barrier, inc=1, device_id=there(dlat, dlon), device_id_type=MESH)

    greet(0, -1)
    greet(0, 1)
    guarded(-1, lambda: greet(-1, 0))
    guarded(1, lambda: greet(1, 0))

    groups = [
        [(snd_h.at[0], snd_v)],
        [
            (mesh_h.at[0, 0], mesh_v),
            (w_mesh_h, w_mesh_v),
            (w_edge_h, w_edge_v),
            (rcv_h.at[0], rcv_v),
            (geo_h.at[0, 0], geo_v),
            (bias_h, bias_v),
            (gain_h, gain_v),
            (nbias_h, nbias_v),
        ],
        [(w_grid_h, w_grid_v), (grid_h.at[0, 0], grid_v)],
        [(w_message_h, w_message_v), (w_node_h, w_node_v), (w_output_h, w_output_v)],
    ]

    def load(number):
        for source, target in groups[number]:
            pltpu.make_async_copy(source, target, load_sem.at[number % 3]).start()

    for number in range(3):
        load(number)

    def bytes_of(ref):
        return ref.dtype.itemsize * functools.reduce(lambda a, b: a * b, ref.shape)

    def await_bytes(total, sem):
        view = ruler.at[:, pl.ds(0, total // ruler.dtype.itemsize)]
        pltpu.make_async_copy(view, view, sem).wait()

    def loaded(number):
        total = sum(bytes_of(target) for _, target in groups[number])
        await_bytes(total, load_sem.at[number % 3])

    def offset(slot):
        return slot // 3 - 1, slot % 3 - 1

    def place(slot):
        if slot in SIDES:
            return rows + B_SIDE * SIDES.index(slot)
        return corner_base + BLOCK * CORNERS.index(slot)

    def size_of(slot):
        return B_SIDE if slot in SIDES else B_CORNER

    def mesh_copy(slot):
        dlat, dlon = offset(slot)
        size = size_of(slot)
        return pltpu.make_async_remote_copy(
            src_ref=table.at[pl.ds(grid_rows + strip(slot) * B_SIDE, size)],
            dst_ref=edge_table.at[pl.ds(place(slot) - cut, size)],
            send_sem=strip_sem.at[0],
            recv_sem=strip_sem.at[1],
            device_id=there(-dlat, -dlon),
            device_id_type=MESH,
        )

    def sum_copy(slot):
        dlat, dlon = offset(slot)
        size = size_of(slot)
        return pltpu.make_async_remote_copy(
            src_ref=put_sum.at[pl.ds(place(slot) - rows, size)],
            dst_ref=got_sum.at[pl.ds(place(slot) - rows, size)],
            send_sem=strip_sem.at[0],
            recv_sem=strip_sem.at[2],
            device_id=there(dlat, dlon),
            device_id_type=MESH,
        )

    bands = (lat > 0).astype(jnp.int32) + (lat < n_lat - 1).astype(jnp.int32)

    def settle(sem, times):
        for count in range(3):

            def body(count=count):
                lines = 2 * B_SIDE + count * (B_SIDE + 2 * B_CORNER)
                await_bytes(times * lines * features * 2, sem)

            pl.when(bands == count)(body)

    def each(chosen, sign, action):
        for dlat in (-1, 0, 1):
            members = [s for s in chosen if offset(s)[0] == sign * dlat]
            if members:

                def body(members=members):
                    for s in members:
                        action(s)

                guarded(dlat, body)

    def send_sides():
        pl.semaphore_wait(barrier, 2 + bands)
        for dlat in (-1, 1):

            def tell(dlat=dlat):
                pl.semaphore_signal(
                    ready_sem.at[0 if dlat > 0 else 1],
                    inc=1,
                    device_id=there(dlat, 0),
                    device_id_type=MESH,
                )

            guarded(dlat, tell)
        each(SIDES, -1, lambda s: mesh_copy(s).start())

    def send_corners(dlat):
        def go():
            pl.semaphore_wait(ready_sem.at[0 if dlat < 0 else 1], 1)
            for s in reversed(CORNERS):
                if offset(s)[0] == -dlat:
                    mesh_copy(s).start()

        guarded(dlat, go)

    step = min(CHUNK, edges)
    starts = list(range(0, edges, step))
    digits = grid_rows // DIGIT
    lane = lax.broadcasted_iota(jnp.int32, (step, LANES), 1).astype(F32)
    lanes = [(lane + float(LANES * h)).astype(BF16) for h in range(DIGIT // LANES)]

    loaded(0)
    senders = snd_v[...]
    upper = lax.shift_left(lax.shift_right_logical(senders, 8), 8)
    lower = (senders - upper).astype(F32).astype(BF16)
    upper = upper.astype(F32).astype(BF16)

    for start in starts:
        span = pl.ds(start, step)
        low_v[span, :] = down(lower[:, start : start + step], LANES)
        high_v[span, :] = down(upper[:, start : start + step], LANES)

    loaded(1)
    high, low = [part.astype(F32) for part in halves(w_edge_v[...])]
    bias_high, bias_low = [part.astype(F32) for part in halves(bias_v[...])]
    blank = jnp.zeros((BLOCK - B_CORNER, features), F32)
    last = jnp.concatenate(
        [bias_high, bias_low, jnp.zeros((B_CORNER - 2, features), F32)], 0
    )
    own = nn(mesh_v[...], w_mesh_v[...])
    table[grid_rows:, :] = (
        0.5
        * jnp.concatenate(
            [own, jnp.zeros((corner_base - rows, features), F32)]
            + [blank, high, blank, low, blank, high, blank, last],
            0,
        )
    ).astype(BF16)
    send_sides()
    send_corners(-1)
    loaded(2)
    load(3)
    table[:grid_rows, :] = (0.5 * nn(grid_v[...], w_grid_v[...])).astype(BF16)

    picks = rcv_v[...]
    shift, spot = 0, picks
    for s in range(9):
        base = (0 if s == 4 else place(s) - strip(s) * B_SIDE) - s * rows
        if s == 0:
            spot = spot + base
        else:
            spot = spot + jnp.where(picks >= s * rows, base - shift, 0)
        shift = base
    spot = spot.astype(F32).astype(BF16)
    high, low = [part.astype(F32) for part in halves(geo_v[...])]
    empty = jnp.zeros((BLOCK - B_CORNER, edges), F32)
    ones = jnp.concatenate([jnp.ones((2, edges), F32), jnp.zeros((2, edges), F32)], 0)
    tail = jnp.concatenate(
        [jnp.zeros((corner_base - cut, edges), F32)]
        + [empty, high, empty, high, empty, low, empty, ones],
        0,
    ).astype(BF16)
    for number, start in enumerate(starts):
        if number == UP_AT:
            send_corners(1)
        span = pl.ds(start, step)
        at = down(spot[:, start : start + step], LANES)
        tiles = []
        for q in range(digits):
            digit = (high_v[span, :] - float(DIGIT * q)) + low_v[span, :]
            tiles += [equal(digit, lanes[h]) for h in range(DIGIT // LANES)]
        for h in range(slots // LANES):
            found = equal(at, lanes[h])
            if h * LANES == cut:
                twice = found.astype(F8)
                picks_8[span, :] = jnp.concatenate([twice, twice], 1)
                found = found + jnp.transpose(tail[:, start : start + step])
            tiles.append(found)
        before[span, :] = nn(jnp.concatenate(tiles, 1), table[...])

    settle(strip_sem.at[1], 1)

    arrived = edge_table[...].astype(F32)
    rough = arrived.astype(F8)
    fine = (arrived - rough.astype(F32)).astype(F8)
    split = jnp.concatenate([rough, fine], 0)
    def gathered(first, count, begin, hidden):
        width = hidden.shape[0]
        row = lax.broadcasted_iota(jnp.int32, (count, width), 0) + first
        at = jnp.broadcast_to(spot[:, begin : begin + width], (count, width))
        return nn(equal(row.astype(F32).astype(BF16), at), hidden)

    unit = edges // sum(BURSTS)
    sizes = [unit * count for count in BURSTS]
    begins = [sum(sizes[:number]) for number in range(len(sizes))]
    halves_of, parts, summed = [], [], None
    for number in range(len(sizes) + LAG):
        if number < len(sizes):
            span = pl.ds(begins[number], sizes[number])
            half = before[span, :] + nn(picks_8[span, :], split)
            halves_of.append(half)
        if 1 <= number <= len(sizes):
            half = halves_of[number - 1]
            parts.append((half + half * jnp.tanh(half)).astype(BF16))
        if number >= LAG:
            done = number - LAG
            added = gathered(rows, slots - rows, begins[done], parts[done])
            summed = added if summed is None else summed + added

    put_sum[...] = summed.astype(BF16)
    each(SENT, 1, lambda s: sum_copy(s).start())

    loaded(3)
    fold = nn(w_message_v[...], w_node_v[features:, :]).astype(BF16)
    high, low = halves(gathered(0, rows, 0, jnp.concatenate(parts, 0)))
    node_v[...] = (
        nn(mesh_v[...], w_node_v[:features, :]) + nn(high, fold) + nn(low, fold)
    )
    weights = w_output_v[...].astype(F32)
    center = jnp.mean(weights, axis=-1, keepdims=True)
    w_center[...] = (weights - center).astype(BF16)

    def rows_of(ref, spans):
        return jnp.concatenate([ref[pl.ds(*span), :].astype(F32) for span in spans], 0)

    def finish(spans, extra=None):
        node = rows_of(node_v, spans)
        if extra is not None:
            node = node + nn(extra[...], fold)
        node_hidden = (node * jax.nn.sigmoid(node)).astype(BF16)
        centered = nn(node_hidden, w_center[...])
        row_var = jnp.mean(centered * centered, axis=-1, keepdims=True)
        normed = centered * lax.rsqrt(row_var + 1e-05) * gain_v[...] + nbias_v[...]
        result = rows_of(mesh_v, spans) + normed
        first = 0
        for start, count in spans:
            out_ref[0, 0, pl.ds(start, count), :] = result[first : first + count].astype(BF16)
            first += count

    at_sides = [(strip(s) * B_SIDE, B_SIDE) for s in SIDES]
    at_corners = [(strip(s) * B_SIDE, BLOCK) for s in CORNERS]
    between = [(strip(s) * B_SIDE + BLOCK, B_SIDE - BLOCK) for s in CORNERS]
    finish([(border, rows - border)] + between)
    settle(strip_sem.at[2], 1)
    finish(at_sides + at_corners, got_sum)

    settle(strip_sem.at[0], 2)


def local(n_lon, n_lat, *args):
    args = [a.reshape(1, -1) if a.ndim == 1 else a for a in args]
    grid_latent, mesh_latent, geometry, senders = args[:4]
    rows, features = mesh_latent.shape[2:]
    grid_rows = grid_latent.shape[2]
    edges = senders.shape[2]
    slots = rows + 4 * B_SIDE + 4 * BLOCK
    cut = rows // LANES * LANES
    ruler = sum(a.size * a.dtype.itemsize for a in args[9:12]) // 4
    loads = []
    for number, a in enumerate(args):
        shape = a.shape[2:] if number < 3 else a.shape[1:] if number < 5 else a.shape
        loads.append(pltpu.VMEM(shape, a.dtype))
    return pl.pallas_call(
        functools.partial(kernel, n_lon, n_lat),
        out_shape=pltpu.VMEM(mesh_latent.shape, BF16),
        in_specs=[pl.BlockSpec(memory_space=pl.ANY)] * len(args),
        out_specs=pl.BlockSpec(memory_space=pltpu.VMEM),
        scratch_shapes=loads
        + [
            pltpu.VMEM((grid_rows + slots, features), BF16),
            pltpu.VMEM((slots - cut, features), BF16),
            pltpu.VMEM((edges, LANES), BF16),
            pltpu.VMEM((edges, LANES), BF16),
            pltpu.VMEM((edges, 2 * LANES), F8),
            pltpu.VMEM((edges, features), F32),
            pltpu.VMEM((slots - rows, features), BF16),
            pltpu.VMEM((slots - rows, features), BF16),
            pltpu.VMEM((features, features), BF16),
            pltpu.VMEM((rows, features), F32),
            pltpu.VMEM((1, ruler), jnp.int32),
            pltpu.SemaphoreType.DMA((3,)),
            pltpu.SemaphoreType.DMA((3,)),
            pltpu.SemaphoreType.REGULAR((2,)),
        ],
        compiler_params=pltpu.CompilerParams(
            collective_id=0, has_side_effects=True, vmem_limit_bytes=56 * 1024 * 1024
        ),
    )(*args)


def solution(mesh):
    return jax.shard_map(
        functools.partial(local, mesh.shape["lon"], mesh.shape["lat"]),
        mesh=mesh,
        in_specs=(
            P("lat", "lon", None, None),
            P("lat", "lon", None, None),
            P("lat", "lon", None, None),
            P("lat", "lon", None),
            P("lat", "lon", None),
            P(),
            P(),
            P(),
            P(),
            P(),
            P(),
            P(),
            P(),
            P(),
        ),
        out_specs=P("lat", "lon", None, None),
        check_vma=False,
    )
```

```python
import functools

import jax
import jax.numpy as jnp
from jax import lax
from jax.experimental import pallas as pl
from jax.experimental.pallas import tpu as pltpu
from jax.sharding import PartitionSpec as P

B_SIDE = 16
B_CORNER = 4
BLOCK = 8
LANES = 128
DIGIT = 256
CHUNK = 256
UP_AT = 1
BURSTS = (1, 1, 2, 2, 2)
LAG = 1
MESH = pl.DeviceIdType.MESH

BF16 = jnp.bfloat16
F32 = jnp.float32

SIDES = (1, 3, 5, 7)
CORNERS = (0, 2, 6, 8)
SENT = (2, 1, 0, 3, 5, 7, 8, 6)


def strip(slot):
    return slot if slot < 4 else slot - 1


def nn(a, b):
    return jnp.dot(a, b, preferred_element_type=F32)


def halves(x):
    high = x.astype(BF16)
    return high, (x - high.astype(F32)).astype(BF16)


def down(row, count):
    return jnp.transpose(jnp.broadcast_to(row, (count, row.shape[1])))


def equal(a, b):
    one = jnp.ones(a.shape, BF16)
    return jnp.where(a == b, one, jnp.zeros_like(one))


def kernel(
    n_lon,
    n_lat,
    grid_h,
    mesh_h,
    geo_h,
    snd_h,
    rcv_h,
    w_grid_h,
    w_mesh_h,
    w_edge_h,
    bias_h,
    w_message_h,
    w_node_h,
    w_output_h,
    gain_h,
    nbias_h,
    out_ref,
    grid_v,
    mesh_v,
    geo_v,
    snd_v,
    rcv_v,
    w_grid_v,
    w_mesh_v,
    w_edge_v,
    bias_v,
    w_message_v,
    w_node_v,
    w_output_v,
    gain_v,
    nbias_v,
    table,
    edge_table,
    low_v,
    high_v,
    picks_v,
    before,
    put_sum,
    got_sum,
    w_center,
    node_v,
    ruler,
    load_sem,
    strip_sem,
    ready_sem,
):
    lon = lax.axis_index("lon")
    lat = lax.axis_index("lat")
    rows, features = mesh_v.shape
    grid_rows = grid_v.shape[0]
    edges = snd_v.shape[1]
    corner_base = rows + 4 * B_SIDE
    slots = corner_base + 4 * BLOCK
    cut = rows // LANES * LANES
    border = 8 * B_SIDE

    def there(dlat, dlon):
        return {
            "lat": lat + dlat,
            "lon": lax.rem(lon + dlon + n_lon, n_lon),
        }

    def guarded(dlat, body):
        if dlat == 0:
            body()
        else:
            pl.when(lat > 0 if dlat < 0 else lat < n_lat - 1)(body)

    edge_table[...] = jnp.zeros(edge_table.shape, BF16)
    got_sum[...] = jnp.zeros(got_sum.shape, BF16)

    barrier = pltpu.get_barrier_semaphore()

    def greet(dlat, dlon):
        pl.semaphore_signal(barrier, inc=1, device_id=there(dlat, dlon), device_id_type=MESH)

    greet(0, -1)
    greet(0, 1)
    guarded(-1, lambda: greet(-1, 0))
    guarded(1, lambda: greet(1, 0))

    groups = [
        [(snd_h.at[0], snd_v)],
        [
            (mesh_h.at[0, 0], mesh_v),
            (w_mesh_h, w_mesh_v),
            (w_edge_h, w_edge_v),
            (rcv_h.at[0], rcv_v),
            (geo_h.at[0, 0], geo_v),
            (bias_h, bias_v),
            (gain_h, gain_v),
            (nbias_h, nbias_v),
        ],
        [(w_grid_h, w_grid_v), (grid_h.at[0, 0], grid_v)],
        [(w_message_h, w_message_v), (w_node_h, w_node_v), (w_output_h, w_output_v)],
    ]

    def load(number):
        for source, target in groups[number]:
            pltpu.make_async_copy(source, target, load_sem.at[number % 3]).start()

    for number in range(3):
        load(number)

    def bytes_of(ref):
        return ref.dtype.itemsize * functools.reduce(lambda a, b: a * b, ref.shape)

    def await_bytes(total, sem):
        view = ruler.at[:, pl.ds(0, total // ruler.dtype.itemsize)]
        pltpu.make_async_copy(view, view, sem).wait()

    def loaded(number):
        total = sum(bytes_of(target) for _, target in groups[number])
        await_bytes(total, load_sem.at[number % 3])

    def offset(slot):
        return slot // 3 - 1, slot % 3 - 1

    def place(slot):
        if slot in SIDES:
            return rows + B_SIDE * SIDES.index(slot)
        return corner_base + BLOCK * CORNERS.index(slot)

    def size_of(slot):
        return B_SIDE if slot in SIDES else B_CORNER

    def mesh_copy(slot):
        dlat, dlon = offset(slot)
        size = size_of(slot)
        return pltpu.make_async_remote_copy(
            src_ref=table.at[pl.ds(grid_rows + strip(slot) * B_SIDE, size)],
            dst_ref=edge_table.at[pl.ds(place(slot) - cut, size)],
            send_sem=strip_sem.at[0],
            recv_sem=strip_sem.at[1],
            device_id=there(-dlat, -dlon),
            device_id_type=MESH,
        )

    def sum_copy(slot):
        dlat, dlon = offset(slot)
        size = size_of(slot)
        return pltpu.make_async_remote_copy(
            src_ref=put_sum.at[pl.ds(place(slot) - rows, size)],
            dst_ref=got_sum.at[pl.ds(place(slot) - rows, size)],
            send_sem=strip_sem.at[0],
            recv_sem=strip_sem.at[2],
            device_id=there(dlat, dlon),
            device_id_type=MESH,
        )

    bands = (lat > 0).astype(jnp.int32) + (lat < n_lat - 1).astype(jnp.int32)

    def settle(sem, times):
        for count in range(3):

            def body(count=count):
                lines = 2 * B_SIDE + count * (B_SIDE + 2 * B_CORNER)
                await_bytes(times * lines * features * 2, sem)

            pl.when(bands == count)(body)

    def each(chosen, sign, action):
        for dlat in (-1, 0, 1):
            members = [s for s in chosen if offset(s)[0] == sign * dlat]
            if members:

                def body(members=members):
                    for s in members:
                        action(s)

                guarded(dlat, body)

    def send_sides():
        pl.semaphore_wait(barrier, 2 + bands)
        for dlat in (-1, 1):

            def tell(dlat=dlat):
                pl.semaphore_signal(
                    ready_sem.at[0 if dlat > 0 else 1],
                    inc=1,
                    device_id=there(dlat, 0),
                    device_id_type=MESH,
                )

            guarded(dlat, tell)
        each(SIDES, -1, lambda s: mesh_copy(s).start())

    def send_corners(dlat):
        def go():
            pl.semaphore_wait(ready_sem.at[0 if dlat < 0 else 1], 1)
            for s in reversed(CORNERS):
                if offset(s)[0] == -dlat:
                    mesh_copy(s).start()

        guarded(dlat, go)

    step = min(CHUNK, edges)
    starts = list(range(0, edges, step))
    digits = grid_rows // DIGIT
    lane = lax.broadcasted_iota(jnp.int32, (step, LANES), 1).astype(F32)
    lanes = [(lane + float(LANES * h)).astype(BF16) for h in range(DIGIT // LANES)]

    loaded(0)
    senders = snd_v[...]
    upper = lax.shift_left(lax.shift_right_logical(senders, 8), 8)
    lower = (senders - upper).astype(F32).astype(BF16)
    upper = upper.astype(F32).astype(BF16)

    for start in starts:
        span = pl.ds(start, step)
        low_v[span, :] = down(lower[:, start : start + step], LANES)
        high_v[span, :] = down(upper[:, start : start + step], LANES)

    loaded(1)
    high, low = [part.astype(F32) for part in halves(w_edge_v[...])]
    bias_high, bias_low = [part.astype(F32) for part in halves(bias_v[...])]
    blank = jnp.zeros((BLOCK - B_CORNER, features), F32)
    last = jnp.concatenate(
        [bias_high, bias_low, jnp.zeros((B_CORNER - 2, features), F32)], 0
    )
    own = nn(mesh_v[...], w_mesh_v[...])
    table[grid_rows:, :] = (
        0.5
        * jnp.concatenate(
            [own, jnp.zeros((corner_base - rows, features), F32)]
            + [blank, high, blank, low, blank, high, blank, last],
            0,
        )
    ).astype(BF16)
    send_sides()
    send_corners(-1)
    loaded(2)
    load(3)
    table[:grid_rows, :] = (0.5 * nn(grid_v[...], w_grid_v[...])).astype(BF16)

    picks = rcv_v[...]
    shift, spot = 0, picks
    for s in range(9):
        base = (0 if s == 4 else place(s) - strip(s) * B_SIDE) - s * rows
        if s == 0:
            spot = spot + base
        else:
            spot = spot + jnp.where(picks >= s * rows, base - shift, 0)
        shift = base
    spot = spot.astype(F32).astype(BF16)
    high, low = [part.astype(F32) for part in halves(geo_v[...])]
    empty = jnp.zeros((BLOCK - B_CORNER, edges), F32)
    ones = jnp.concatenate([jnp.ones((2, edges), F32), jnp.zeros((2, edges), F32)], 0)
    tail = jnp.concatenate(
        [jnp.zeros((corner_base - cut, edges), F32)]
        + [empty, high, empty, high, empty, low, empty, ones],
        0,
    ).astype(BF16)
    for number, start in enumerate(starts):
        if number == UP_AT:
            send_corners(1)
        span = pl.ds(start, step)
        at = down(spot[:, start : start + step], LANES)
        tiles = []
        for q in range(digits):
            digit = (high_v[span, :] - float(DIGIT * q)) + low_v[span, :]
            tiles += [equal(digit, lanes[h]) for h in range(DIGIT // LANES)]
        for h in range(slots // LANES):
            found = equal(at, lanes[h])
            if h * LANES == cut:
                found = found + jnp.transpose(tail[:, start : start + step])
            picks_v[span, pl.ds(h * LANES, LANES)] = found
        before[span, :] = nn(jnp.concatenate(tiles, 1), table[:grid_rows, :])

    settle(strip_sem.at[1], 1)

    first = grid_rows + rows
    table[first:, :] = table[first:, :] + edge_table[rows - cut :, :]

    def gathered(first, count, begin, hidden):
        width = hidden.shape[0]
        row = lax.broadcasted_iota(jnp.int32, (count, width), 0) + first
        at = jnp.broadcast_to(spot[:, begin : begin + width], (count, width))
        return nn(equal(row.astype(F32).astype(BF16), at), hidden)

    unit = edges // sum(BURSTS)
    sizes = [unit * count for count in BURSTS]
    begins = [sum(sizes[:number]) for number in range(len(sizes))]
    halves_of, parts, summed = [], [], None
    for number in range(len(sizes) + LAG):
        if number < len(sizes):
            span = pl.ds(begins[number], sizes[number])
            half = before[span, :] + nn(picks_v[span, :], table[grid_rows:, :])
            halves_of.append(half)
        if 1 <= number <= len(sizes):
            half = halves_of[number - 1]
            parts.append((half + half * jnp.tanh(half)).astype(BF16))
        if number >= LAG:
            done = number - LAG
            added = gathered(rows, slots - rows, begins[done], parts[done])
            summed = added if summed is None else summed + added

    put_sum[...] = summed.astype(BF16)
    each(SENT, 1, lambda s: sum_copy(s).start())

    loaded(3)
    fold = nn(w_message_v[...], w_node_v[features:, :]).astype(BF16)
    high, low = halves(gathered(0, rows, 0, jnp.concatenate(parts, 0)))
    node_v[...] = (
        nn(mesh_v[...], w_node_v[:features, :]) + nn(high, fold) + nn(low, fold)
    )
    weights = w_output_v[...].astype(F32)
    center = jnp.mean(weights, axis=-1, keepdims=True)
    w_center[...] = (weights - center).astype(BF16)

    def rows_of(ref, spans):
        return jnp.concatenate([ref[pl.ds(*span), :].astype(F32) for span in spans], 0)

    def finish(spans, extra=None):
        node = rows_of(node_v, spans)
        if extra is not None:
            node = node + nn(extra[...], fold)
        node_hidden = (node * jax.nn.sigmoid(node)).astype(BF16)
        centered = nn(node_hidden, w_center[...])
        row_var = jnp.mean(centered * centered, axis=-1, keepdims=True)
        normed = centered * lax.rsqrt(row_var + 1e-05) * gain_v[...] + nbias_v[...]
        result = rows_of(mesh_v, spans) + normed
        first = 0
        for start, count in spans:
            out_ref[0, 0, pl.ds(start, count), :] = result[first : first + count].astype(BF16)
            first += count

    at_sides = [(strip(s) * B_SIDE, B_SIDE) for s in SIDES]
    at_corners = [(strip(s) * B_SIDE, BLOCK) for s in CORNERS]
    between = [(strip(s) * B_SIDE + BLOCK, B_SIDE - BLOCK) for s in CORNERS]
    finish([(border, rows - border)] + between)
    settle(strip_sem.at[2], 1)
    finish(at_sides + at_corners, got_sum)

    settle(strip_sem.at[0], 2)


def local(n_lon, n_lat, *args):
    args = [a.reshape(1, -1) if a.ndim == 1 else a for a in args]
    grid_latent, mesh_latent, geometry, senders = args[:4]
    rows, features = mesh_latent.shape[2:]
    grid_rows = grid_latent.shape[2]
    edges = senders.shape[2]
    slots = rows + 4 * B_SIDE + 4 * BLOCK
    cut = rows // LANES * LANES
    ruler = sum(a.size * a.dtype.itemsize for a in args[9:12]) // 4
    loads = []
    for number, a in enumerate(args):
        shape = a.shape[2:] if number < 3 else a.shape[1:] if number < 5 else a.shape
        loads.append(pltpu.VMEM(shape, a.dtype))
    return pl.pallas_call(
        functools.partial(kernel, n_lon, n_lat),
        out_shape=pltpu.VMEM(mesh_latent.shape, BF16),
        in_specs=[pl.BlockSpec(memory_space=pl.ANY)] * len(args),
        out_specs=pl.BlockSpec(memory_space=pltpu.VMEM),
        scratch_shapes=loads
        + [
            pltpu.VMEM((grid_rows + slots, features), BF16),
            pltpu.VMEM((slots - cut, features), BF16),
            pltpu.VMEM((edges, LANES), BF16),
            pltpu.VMEM((edges, LANES), BF16),
            pltpu.VMEM((edges, slots), BF16),
            pltpu.VMEM((edges, features), F32),
            pltpu.VMEM((slots - rows, features), BF16),
            pltpu.VMEM((slots - rows, features), BF16),
            pltpu.VMEM((features, features), BF16),
            pltpu.VMEM((rows, features), F32),
            pltpu.VMEM((1, ruler), jnp.int32),
            pltpu.SemaphoreType.DMA((3,)),
            pltpu.SemaphoreType.DMA((3,)),
            pltpu.SemaphoreType.REGULAR((2,)),
        ],
        compiler_params=pltpu.CompilerParams(
            collective_id=0, has_side_effects=True, vmem_limit_bytes=56 * 1024 * 1024
        ),
    )(*args)


def solution(mesh):
    return jax.shard_map(
        functools.partial(local, mesh.shape["lon"], mesh.shape["lat"]),
        mesh=mesh,
        in_specs=(
            P("lat", "lon", None, None),
            P("lat", "lon", None, None),
            P("lat", "lon", None, None),
            P("lat", "lon", None),
            P("lat", "lon", None),
            P(),
            P(),
            P(),
            P(),
            P(),
            P(),
            P(),
            P(),
            P(),
        ),
        out_specs=P("lat", "lon", None, None),
        check_vma=False,
    )
```
